32 devices in a mesh: dp: 8 (over z, y), tensor: 4 (over x, core).
Axes of the slice: x: 2, y: 2, z: 4, core: 2. Of those that a mesh axis runs over, the one named last changes fastest.
Arguments:
- patches: bfloat16 [8192, 1280], P('dp'), may hold values from -27 to 27
- norm_gain: float32 [1280], replicated, may hold values from 0.1 to 1.9
- norm_bias: float32 [1280], replicated, may hold values from -3 to 3
- first_weight: bfloat16 [5120, 5120], P(None, 'tensor'), may hold values from -0.078125 to 0.078125
- first_bias: float32 [5120], P('tensor'), may hold values from -3 to 3
- second_weight: bfloat16 [5120, 8192], P('tensor', 'dp'), may hold values from -0.078125 to 0.078125
- second_bias: float32 [8192], P('tensor'), may hold values from -2 to 2
- text_embeds: bfloat16 [4096, 8192], P('dp', 'tensor'), may hold values from -36 to 36
- final_gain: float32 [8192], P('tensor'), may hold values from 0.1 to 1.9
- image_grids: int32 [8, 4, 2], replicated, may hold values from 2 to 8, as said below
- routing: int32 [8, 4], replicated, may hold values from 0 to 3, each once within a row
Outputs:
- embeddings: bfloat16 [4096, 8192], P('dp', 'tensor')
- normed: bfloat16 [4096, 8192], P('dp', 'tensor')
The draws below stay inside these ranges and needn't reach their ends.
Inputs may be any that keep to these rules, and one draw needn't show every extreme that they name: `image_grids`: each image is a grid of 3 to 8 rows by 2 to 8 columns of merged tokens; in every draw some image is 8 by 8. `routing`: each row names every offset 0 to 3 once.
All inputs are finite; a program needn't handle non-finite values.
Results may differ from the reference program's by a relative error of at most 0.006.
Values may be sent and summed in bfloat16 or wider, within the bound.
A program may use at most 128 MiB of HBM per device.

```python
import jax
import jax.numpy as jnp
from jax import lax

D_VIT = 1280
D = 8192
D_MERGE = 5120
BLOCKS = 4
SLOTS = 256
CAP = 64
SEQ = 512
SHARDS = 8
PATCHES = 8192
TOTAL_SEQ = 4096
N_TENSOR = 4


def draw_patches(key, part):
    keys = jax.random.split(jax.random.fold_in(key, 11), 3)
    row_scale = jnp.exp(jax.random.uniform(keys[1], (PATCHES, 1), jnp.float32, jnp.log(0.5), jnp.log(5.0)))
    row_offset = jax.random.uniform(keys[2], (PATCHES, 1), jnp.float32, -1.0, 1.0)
    base = jax.random.normal(keys[0], (PATCHES, D_VIT), jnp.float32)
    base = jnp.clip(base, -5.0, 5.0)
    return (base * row_scale + row_offset).astype(jnp.bfloat16)


def draw_text_embeds(key, part):
    keys = jax.random.split(jax.random.fold_in(key, 23), 3)
    column_ids = jnp.arange(D, dtype=jnp.float32)
    column_scale = 0.6 * jnp.power(3.0, column_ids / (D - 1)) * jax.random.uniform(keys[1], (D,), jnp.float32, 0.7, 1.3)
    row_scale = jnp.exp(jax.random.uniform(keys[2], (TOTAL_SEQ, 1), jnp.float32, jnp.log(0.3), jnp.log(3.0)))
    base = jax.random.normal(keys[0], (TOTAL_SEQ, D), jnp.float32)
    base = jnp.clip(base, -5.0, 5.0)
    return (base * row_scale * column_scale[None, :]).astype(jnp.bfloat16)


def draw_image_grids(key, part):
    keys = jax.random.split(jax.random.fold_in(key, 37), 4)
    grid_rows = jax.random.randint(keys[0], (SHARDS, BLOCKS), 3, 9)
    grid_columns = jax.random.randint(keys[1], (SHARDS, BLOCKS), 2, CAP // 8 + 1)
    full_shard = jax.random.randint(keys[2], (), 0, SHARDS)
    full_block = jax.random.randint(keys[3], (), 0, BLOCKS)
    shard_ids = jnp.arange(SHARDS, dtype=jnp.int32)[:, None]
    block_ids = jnp.arange(BLOCKS, dtype=jnp.int32)[None, :]
    target = (shard_ids == full_shard) & (block_ids == full_block)
    grid_rows = jnp.where(target, 8, grid_rows)
    grid_columns = jnp.where(target, CAP // 8, grid_columns)
    return jnp.stack([grid_rows, grid_columns], axis=-1).astype(jnp.int32)


def levels(own_key, shape, pieces, smallest, largest):
    def one(dim, shards_of):
        steps = jax.random.uniform(jax.random.fold_in(jax.random.fold_in(own_key, 6), dim), (shards_of,), jnp.float32, smallest / len(pieces), largest / len(pieces))
        return jnp.repeat(jnp.exp(steps), shape[dim] // shards_of).reshape((-1,) + (1,) * (len(shape) - dim - 1))

    loudness = one(*pieces[0])
    for cut in pieces[1:]:
        loudness = loudness * one(*cut)
    return loudness


def normal_values(own_key, shape, width, most, cuts=(), kind=jnp.bfloat16):
    level = levels(own_key, shape, cuts, -0.22, 0.18) if cuts else 1.0
    drawn = jax.random.normal(own_key, shape, jnp.float32) * width * level
    return jnp.minimum(jnp.maximum(drawn, -most), most).astype(kind)


def setup_inputs(seed: int = 0) -> dict:
    seeds = jax.random.split(jax.random.key(seed), 12)
    patches = draw_patches(jax.random.fold_in(seeds[11], 71), 0)
    norm_gain = jnp.clip(1.0 + 0.18 * jax.random.normal(seeds[1], (D_VIT,), jnp.float32), 0.1, 1.9)
    norm_bias = normal_values(seeds[2], (D_VIT,), 0.5, 3.0, (), jnp.float32)
    first_weight = normal_values(seeds[3], (D_MERGE, D_MERGE), D_MERGE ** -0.5, 0.078125, ((1, 4),))
    first_bias = normal_values(seeds[4], (D_MERGE,), 0.5, 3.0, ((0, 4),), jnp.float32)
    second_weight = normal_values(seeds[5], (D_MERGE, D), D_MERGE ** -0.5, 0.078125, ((0, 4), (1, 8)))
    second_bias = normal_values(seeds[6], (D,), 0.3, 2.0, ((0, 4),), jnp.float32)
    text_embeds = draw_text_embeds(jax.random.fold_in(seeds[11], 71), 0)
    final_gain = jnp.clip(1.0 + 0.18 * jax.random.normal(seeds[8], (D,), jnp.float32), 0.1, 1.9)
    image_grids = draw_image_grids(jax.random.fold_in(seeds[11], 71), 0)
    routing = jax.vmap(lambda own: jax.random.permutation(own, BLOCKS))(jax.random.split(seeds[10], SHARDS)).reshape((SHARDS, BLOCKS)).astype(jnp.int32)
    return {"patches": patches, "norm_gain": norm_gain, "norm_bias": norm_bias, "first_weight": first_weight, "first_bias": first_bias, "second_weight": second_weight, "second_bias": second_bias, "text_embeds": text_embeds, "final_gain": final_gain, "image_grids": image_grids, "routing": routing}


def reference(patches, norm_gain, norm_bias, first_weight, first_bias, second_weight, second_bias, text_embeds, final_gain, image_grids, routing):
    patch_values = patches.astype(jnp.float32)
    centered = patch_values - lax.optimization_barrier(jnp.mean(patch_values, axis=-1, keepdims=True))
    variance = lax.optimization_barrier(jnp.mean(centered * centered, axis=-1, keepdims=True))
    normed_patches = centered * lax.rsqrt(variance + 1e-06) * norm_gain + norm_bias
    merged = normed_patches.reshape(-1, D_MERGE).astype(jnp.bfloat16)
    hidden = jax.nn.gelu(jnp.dot(merged, first_weight, preferred_element_type=jnp.float32) + first_bias, approximate=False).astype(jnp.bfloat16)
    group_width = D_MERGE // N_TENSOR
    summed = jnp.zeros((hidden.shape[0], D), jnp.float32)
    for group in range(N_TENSOR):
        partial_value = jnp.dot(hidden[:, group * group_width:(group + 1) * group_width], second_weight[group * group_width:(group + 1) * group_width], preferred_element_type=jnp.float32).astype(jnp.bfloat16)
        partial_value = lax.optimization_barrier(partial_value)
        summed = summed + partial_value.astype(jnp.float32)
    projected = (summed + second_bias).astype(jnp.bfloat16)
    counts_all = (image_grids[:, :, 0] * image_grids[:, :, 1]).astype(jnp.int32)
    shard_ids = jnp.arange(SHARDS, dtype=jnp.int32)[:, None]
    stride_ids = jnp.arange(BLOCKS, dtype=jnp.int32)[None, :]
    source_shard = ((shard_ids - stride_ids) % SHARDS).astype(jnp.int32)
    source_routing = routing[source_shard]
    block_ids = jnp.arange(BLOCKS, dtype=jnp.int32)[None, None, :]
    chosen = lax.optimization_barrier(jnp.sum(jnp.where(source_routing == stride_ids[:, :, None], block_ids, 0), axis=-1)).astype(jnp.int32)
    lengths = counts_all[source_shard, chosen]
    starts = (jnp.cumsum(lengths, axis=1) - lengths).astype(jnp.int32)
    totals = lax.optimization_barrier(jnp.sum(lengths, axis=1))
    position = jnp.arange(SEQ, dtype=jnp.int32)[None, :]
    which = lax.optimization_barrier(jnp.sum((position[:, :, None] >= starts[:, None, 1:]).astype(jnp.int32), axis=-1)).astype(jnp.int32)
    start_at = jnp.take_along_axis(starts, which, axis=1)
    source_at = jnp.take_along_axis(source_shard, which, axis=1)
    chosen_at = jnp.take_along_axis(chosen, which, axis=1)
    valid = position < totals[:, None]
    row_index = jnp.where(valid, source_at * SLOTS + chosen_at * CAP + position - start_at, 0).astype(jnp.int32)
    image_rows = jnp.take(projected, row_index.reshape(-1), axis=0).reshape(SHARDS, SEQ, D)
    text_rows = text_embeds.reshape(SHARDS, SEQ, D)
    embeddings = jnp.where(valid[:, :, None], image_rows, text_rows).reshape(SHARDS * SEQ, D)
    embed_values = embeddings.astype(jnp.float32)
    mean_square = lax.optimization_barrier(jnp.mean(embed_values * embed_values, axis=-1, keepdims=True))
    normed = (embed_values * lax.rsqrt(mean_square + 1e-06) * final_gain).astype(jnp.bfloat16)
    return (embeddings, normed)
```

```python
import functools

import jax
import jax.numpy as jnp
from jax import lax
from jax.experimental import pallas as pl
from jax.experimental.pallas import tpu as pltpu
from jax.sharding import PartitionSpec as P

VMEM_LIMIT = 62 * 1024 * 1024
LANES = 128
CHUNK = 256
F32 = jnp.float32
BF16 = jnp.bfloat16


def area_of(grids_ref, s, b):
    return grids_ref[s, b, 0] * grids_ref[s, b, 1]


def segment(grids_ref, routing_ref, s, k):
    count, start = jnp.int32(0), jnp.int32(0)
    for b in range(routing_ref.shape[1]):
        area, offset = area_of(grids_ref, s, b), routing_ref[s, b]
        count = count + jnp.where(offset == k, area, 0)
        start = start + jnp.where(offset < k, area, 0)
    return count, start


def plan_kernel(buckets, grids_ref, routing_ref, which_ref):
    shards, strides = routing_ref.shape

    def widest(e, most):
        sent, filled = jnp.int32(0), jnp.int32(0)
        for k in range(strides):
            sent = sent + area_of(grids_ref, e, k)
            filled = filled + segment(grids_ref, routing_ref, (e + shards - k) % shards, k)[0]
        return jnp.maximum(most, jnp.maximum(sent, filled))

    most = lax.fori_loop(0, shards, widest, jnp.int32(0))
    which = jnp.int32(0)
    for bucket in buckets[:-1]:
        which = which + (most > bucket).astype(jnp.int32)
    which_ref[0] = which


def merge_kernel(
    rows, by_columns,
    grids_ref, routing_ref, patches_ref, gain_ref, bias_ref, first_ref, first_bias_ref, second_ref, second_bias_ref, text_ref,
    out_ref, sums_ref,
    patch_buf, merged, first_buf, second_buf, text_buf, own_pick, acc, gath, proj,
    part, pair_in, cross_out, cross_in, ready_buf, wide, sums_out, sums_in,
    patch_sem, first_sem, second_sem, text_sem,
    line_send, line_recv, pair_send, pair_recv, swap_send, swap_recv, cross_send, cross_recv,
    wide_send, wide_recv, out_send, out_recv, sums_send, sums_recv,
):
    shards, chunks = gath.shape[0], gath.shape[1]
    strides = routing_ref.shape[1]
    groups, piece_rows, piece_cols = part.shape[1:]
    per_group = shards // groups
    length = shards // 2
    per_token, tokens, vit = merged.shape
    cap = tokens // strides
    depth, width = second_buf.shape
    span_width = min(CHUNK, width)
    spans = width // span_width
    ln_rows = LANES
    ln_steps = patch_buf.shape[0] // ln_rows
    ln_tokens = ln_rows // per_token
    seq = text_buf.shape[0]
    feature = text_buf.shape[1]
    top_rows = out_ref.shape[0]

    me = lax.axis_index("dp")
    group = lax.axis_index("tensor")
    place, row = me // 2, me % 2
    other = me + 1 - 2 * row
    core, side = group % 2, group // 2
    mate = 2 * side + 1 - core
    across = group + 2 - 4 * side
    across_mate = mate + 2 - 4 * side
    peers = (mate, across, across_mate)

    barrier = pltpu.get_barrier_semaphore()
    for peer in peers:
        pl.semaphore_signal(barrier, inc=1, device_id={"tensor": peer})

    def greet(i, carry):
        pl.semaphore_signal(barrier, inc=1, device_id={"dp": (me + 1 + i) % shards})
        return carry

    lax.fori_loop(0, shards - 1, greet, 0)

    def patch_copy(i):
        span = pl.ds(pl.multiple_of(i * ln_rows, ln_rows), ln_rows)
        return pltpu.make_async_copy(patches_ref.at[span, :], patch_buf.at[span, :], patch_sem.at[i])

    def first_copy(c):
        span = pl.ds(pl.multiple_of(c * CHUNK, CHUNK), CHUNK)
        return pltpu.make_async_copy(first_ref.at[:, span], first_buf.at[c], first_sem.at[c])

    second_copy = pltpu.make_async_copy(second_ref, second_buf, second_sem)
    text_copy = pltpu.make_async_copy(text_ref, text_buf, text_sem)

    def start_patch(i, carry):
        patch_copy(i).start()
        return carry

    lax.fori_loop(0, ln_steps, start_patch, 0)

    token_row = lax.broadcasted_iota(jnp.int32, (rows, tokens), 0)
    token_gap = lax.broadcasted_iota(jnp.int32, (rows, tokens), 1) - token_row
    picked = jnp.zeros((rows, tokens), jnp.bool_)
    for b in range(strides):
        offset = routing_ref[me, b]
        start = jnp.int32(0)
        for o in range(strides):
            start = start + jnp.where(routing_ref[me, o] < offset, area_of(grids_ref, me, o), 0)
        stop = start + area_of(grids_ref, me, b)
        picked = picked | ((token_row >= start) & (token_row < stop) & (token_gap == b * cap - start))
    own_pick[...] = picked.astype(F32).astype(BF16)

    gain = gain_ref[...][None, :]
    bias = bias_ref[...][None, :]
    line = lax.broadcasted_iota(jnp.int32, (ln_rows, ln_rows), 0)
    wanted = per_token * (line % ln_tokens) + line // ln_tokens
    regroup = (lax.broadcasted_iota(jnp.int32, (ln_rows, ln_rows), 1) == wanted).astype(F32).astype(BF16)

    def norm_rows(i, carry):
        @pl.when(i < chunks)
        def _():
            first_copy(i).start()

        patch_copy(i).wait()
        span = pl.ds(pl.multiple_of(i * ln_rows, ln_rows), ln_rows)
        values = patch_buf[span, :].astype(F32)
        centered = values - jnp.mean(values, axis=-1, keepdims=True)
        variance = jnp.mean(centered * centered, axis=-1, keepdims=True)
        normed = (centered * lax.rsqrt(variance + 1e-06) * gain + bias).astype(BF16)
        sorted_rows = jnp.dot(regroup, normed, preferred_element_type=F32).astype(BF16)
        for j in range(per_token):
            merged[j, pl.ds(pl.multiple_of(i * ln_tokens, ln_tokens), ln_tokens), :] = sorted_rows[j * ln_tokens:(j + 1) * ln_tokens]
        return carry

    lax.fori_loop(0, ln_steps, norm_rows, 0)
    second_copy.start()
    text_copy.start()
    pl.semaphore_wait(barrier, shards - 1 + len(peers))

    def hidden_chunk(c):
        first_copy(c).wait()

        def add(j, carry):
            weight = first_buf[c, pl.ds(pl.multiple_of(j * vit, vit), vit), :]
            term = jnp.dot(merged[j], weight, preferred_element_type=F32)
            acc[...] = jnp.where(j == 0, term, acc[...] + term)
            return carry

        lax.fori_loop(0, per_token, add, 0)
        x = acc[...] + first_bias_ref[pl.ds(pl.multiple_of(c * CHUNK, CHUNK), CHUNK)][None, :]
        hidden = (0.5 * x * (1.0 + lax.erf(x * (0.5 ** 0.5)))).astype(BF16)
        gath[me, c] = jnp.dot(own_pick[...], hidden, preferred_element_type=F32).astype(BF16)

    def line_copy(block, c, way):
        here = gath.at[2 * block + row, c]
        return pltpu.make_async_remote_copy(
            src_ref=here,
            dst_ref=here,
            send_sem=line_send.at[(way + 1) // 2, block, c],
            recv_sem=line_recv.at[block, c],
            device_id={"dp": me + 2 * way},
        )

    def pair_copy(block, c, side_row):
        here = gath.at[2 * block + side_row, c]
        return pltpu.make_async_remote_copy(
            src_ref=here,
            dst_ref=here,
            send_sem=pair_send.at[block, c],
            recv_sem=pair_recv.at[block, c],
            device_id={"dp": other},
        )

    def swap_copy(e, slot):
        return pltpu.make_async_remote_copy(
            src_ref=part.at[e, mate if slot == 0 else across_mate],
            dst_ref=pair_in.at[e, slot],
            send_sem=swap_send.at[slot, e],
            recv_sem=swap_recv.at[slot, e],
            device_id={"tensor": mate},
        )

    def cross_copy(e):
        return pltpu.make_async_remote_copy(
            src_ref=cross_out.at[e],
            dst_ref=cross_in.at[e],
            send_sem=cross_send.at[e],
            recv_sem=cross_recv.at[e],
            device_id={"tensor": across},
        )

    def wide_copy(e, source):
        return pltpu.make_async_remote_copy(
            src_ref=ready_buf.at[e],
            dst_ref=wide.at[source],
            send_sem=wide_send.at[e],
            recv_sem=wide_recv.at[source],
            device_id={"dp": e},
        )

    def place_of(source, sender):
        if by_columns:
            at = ((source % per_group) * groups + sender) * piece_cols
            return pl.ds(0, rows), pl.ds(pl.multiple_of(at, piece_cols), piece_cols)
        return (
            pl.ds(pl.multiple_of(sender * piece_rows, piece_rows), piece_rows),
            pl.ds(pl.multiple_of((source % per_group) * piece_cols, piece_cols), piece_cols),
        )

    def out_copy(source, target, sender):
        return pltpu.make_async_remote_copy(
            src_ref=wide.at[source],
            dst_ref=out_ref.at[place_of(source, sender)],
            send_sem=out_send.at[source],
            recv_sem=out_recv.at[sender, source % per_group],
            device_id={"tensor": target},
        )

    def ready_step(e, at_place, at_row):
        last = jnp.int32(0)
        for k in range(strides):
            source = (e + shards - k) % shards
            away = jnp.abs(source // 2 - at_place) + 1 + jnp.abs(source % 2 - at_row)
            last = jnp.maximum(last, away)
        return last

    def over_shards(body):
        def run(i, carry):
            body((me + 1 + i) % shards)
            return carry

        lax.fori_loop(0, shards, run, 0)

    def project(source, q):
        left = jnp.concatenate([gath[source, c] for c in range(chunks)], axis=1)
        span = pl.ds(pl.multiple_of(q * span_width, span_width), span_width)
        proj[source, :, span] = jnp.dot(left, second_buf[:, span], preferred_element_type=F32).astype(BF16)

    def pick(e):
        at_row = lax.broadcasted_iota(jnp.int32, (rows, rows), 0)
        gap = lax.broadcasted_iota(jnp.int32, (rows, rows), 1) - at_row
        laid = jnp.int32(0)
        total = None
        for k in range(strides):
            source = (e + shards - k) % shards
            count, start = segment(grids_ref, routing_ref, source, k)
            chosen = (at_row >= laid) & (at_row < laid + count) & (gap == start - laid)
            term = jnp.dot(chosen.astype(F32).astype(BF16), proj[source], preferred_element_type=F32)
            total = term if total is None else total + term
            laid = laid + count
        total = total.astype(BF16)
        for g in range(groups):
            if by_columns:
                part[e, g] = total[:, g * piece_cols:(g + 1) * piece_cols]
            else:
                part[e, g] = total[g * piece_rows:(g + 1) * piece_rows]
        for slot in (1, 0):
            swap_copy(e, slot).start()

    def cross(e):
        swap_copy(e, 1).wait_recv()
        cross_out[e] = (part[e, across].astype(F32) + pair_in[e, 1].astype(F32)).astype(BF16)
        cross_copy(e).start()

    def forward(source):
        target = source // per_group

        @pl.when(target == group)
        def _():
            at_rows, at_cols = place_of(source, group)
            out_ref[at_rows, at_cols] = wide[source]

        @pl.when(target != group)
        def _():
            out_copy(source, target, group).start()

    def finish(e):
        swap_copy(e, 0).wait_recv()
        cross_copy(e).wait_recv()
        total = (part[e, group].astype(F32) + pair_in[e, 0].astype(F32) + cross_in[e].astype(F32)).astype(BF16)

        @pl.when(e != me)
        def _():
            ready_buf[e] = total
            wide_copy(e, me).start()

        @pl.when(e == me)
        def _():
            wide[me] = total
            forward(me)

    def row_sums(values):
        squares = values * values
        lanes = squares[:, :LANES]
        for f in range(1, feature // LANES):
            lanes = lanes + squares[:, f * LANES:(f + 1) * LANES]
        return jnp.sum(lanes.T, axis=0, keepdims=True)

    def text_sums():
        text_copy.wait()

        def block(i, carry):
            span = pl.ds(pl.multiple_of(i * LANES, LANES), LANES)
            sums_out[:, span] = row_sums(text_buf[span, :].astype(F32))
            return carry

        lax.fori_loop(0, seq // LANES, block, 0)

    pick_slot = (spans + 1) // 2
    cross_slot = pick_slot + 1

    def slot_step(step, c):
        @pl.when(step == 0)
        def _():
            hidden_chunk(c)

        for way in (1, -1):
            block = place - way * step
            have = (step < length) & (block >= 0) & (block < length)

            @pl.when(have & (step > 0))
            def _(block=block, way=way):
                line_copy(block, c, way).wait_recv()

            @pl.when(have & (place + way >= 0) & (place + way < length))
            def _(block=block, way=way):
                line_copy(block, c, way).start()

            @pl.when(have & ((step > 0) | (way == 1)))
            def _(block=block):
                pair_copy(block, c, row).start()

        @pl.when((step == 1) & (c == 0))
        def _():
            second_copy.wait()

        @pl.when((step == 1) & (c == cross_slot))
        def _():
            text_sums()

        @pl.when((step == length + 1) & (c == 0))
        def _():
            def early(e):
                @pl.when(ready_step(e, place, row) <= length)
                def _():
                    finish(e)

            over_shards(early)

        @pl.when(c < pick_slot)
        def _():
            def unit(i, carry):
                kind, way = i // 2, 1 - 2 * (i % 2)
                away = step - 1 - kind
                block = place - way * away
                fits = (away >= 0) & ((away > 0) | (way == 1)) & (block >= 0) & (block < length)

                @pl.when(fits)
                def _():
                    source = 2 * block + jnp.abs(row - kind)

                    def part_of(h, carry):
                        project(source, 2 * c + h)
                        return carry

                    lax.fori_loop(0, min(2, spans), part_of, 0)

                return carry

            lax.fori_loop(0, 4, unit, 0)

        @pl.when(c == pick_slot)
        def _():
            def now(e):
                @pl.when(ready_step(e, place, row) == step)
                def _():
                    pick(e)

            over_shards(now)

        @pl.when(c == cross_slot)
        def _():
            def now(e):
                @pl.when(ready_step(e, place, row) == step)
                def _():
                    cross(e)

            over_shards(now)

        for way in (1, -1):
            block = place - way * (step - 1)
            have = (step >= 1) & (step <= length) & (block >= 0) & (block < length)

            @pl.when(have & ((step > 1) | (way == 1)))
            def _(block=block):
                pair_copy(block, c, 1 - row).wait_recv()

    def outer(step, carry):
        def inner(c, carry):
            slot_step(step, c)
            return carry

        return lax.fori_loop(0, chunks, inner, carry)

    lax.fori_loop(0, length + 2, outer, 0)

    def receive(source):
        wide_copy(source, source).wait_recv()
        forward(source)

    def settle(i, carry):
        e = (me + 1 + i) % shards

        @pl.when(ready_step(e, place, row) > length)
        def _():
            finish(e)

        source = (me + 2 * shards - 1 - i) % shards

        @pl.when((source != me) & (ready_step(me, source // 2, source % 2) <= length))
        def _():
            receive(source)

        return carry

    lax.fori_loop(0, shards, settle, 0)

    def late(i, carry):
        source = (me + 2 * shards - 1 - i) % shards

        @pl.when((source != me) & (ready_step(me, source // 2, source % 2) > length))
        def _():
            receive(source)

        return carry

    lax.fori_loop(0, shards, late, 0)

    for peer in peers:

        def arrive(c, carry, peer=peer):
            out_copy(group * per_group + c, peer, peer).wait_recv()
            return carry

        lax.fori_loop(0, per_group, arrive, 0)

    filled = jnp.int32(0)
    for k in range(strides):
        filled = filled + segment(grids_ref, routing_ref, (me + shards - k) % shards, k)[0]

    second_bias = second_bias_ref[...][None, :]
    if rows < top_rows:
        out_ref[rows:, :] = text_buf[rows:top_rows, :]

    def splice(i, carry):
        span = pl.ds(pl.multiple_of(i * LANES, LANES), LANES)
        image = (out_ref[span, :].astype(F32) + second_bias).astype(BF16)
        line = lax.broadcasted_iota(jnp.int32, (LANES, feature), 0) + i * LANES
        values = jnp.where(line < filled, image.astype(F32), text_buf[span, :].astype(F32))
        out_ref[span, :] = values.astype(BF16)
        sums_out[:, span] = row_sums(values)
        return carry

    lax.fori_loop(0, top_rows // LANES, splice, 0)

    def sums_copy(peer, sender, i):
        return pltpu.make_async_remote_copy(
            src_ref=sums_out,
            dst_ref=sums_in.at[sender],
            send_sem=sums_send.at[i],
            recv_sem=sums_recv.at[sender],
            device_id={"tensor": peer},
        )

    for i, peer in enumerate(peers):
        sums_copy(peer, group, i).start()

    def drain_line(t, carry):
        block, c = t // chunks, t % chunks
        pair_copy(block, c, row).wait_send()

        @pl.when((block <= place) & (place < length - 1))
        def _():
            line_copy(block, c, 1).wait_send()

        @pl.when((block >= place) & (place > 0))
        def _():
            line_copy(block, c, -1).wait_send()

        return carry

    lax.fori_loop(0, length * chunks, drain_line, 0)

    def drain(e):
        for slot in (1, 0):
            swap_copy(e, slot).wait_send()
        cross_copy(e).wait_send()

        @pl.when(e != me)
        def _():
            wide_copy(e, me).wait_send()

        @pl.when(e // per_group != group)
        def _():
            out_copy(e, e // per_group, group).wait_send()

    over_shards(drain)
    total = sums_out[...]
    for i, peer in enumerate(peers):
        copy = sums_copy(peer, peer, i)
        copy.wait_recv()
        copy.wait_send()
        total = total + sums_in[peer]
    sums_ref[...] = total


def merge(rows, call_id, shards, groups, grids, routing, patches, norm_gain, norm_bias, first_weight, first_bias, second_weight, second_bias, text_embeds):
    patch_rows, vit = patches.shape
    per_token = first_weight.shape[0] // vit
    tokens = patch_rows // per_token
    hidden_width = first_weight.shape[1]
    chunks = hidden_width // CHUNK
    depth, width = second_weight.shape
    seq, feature = text_embeds.shape
    length = shards // 2
    by_columns = width % (groups * LANES) == 0
    piece = (rows, width // groups) if by_columns else (rows // groups, width)
    per_group = shards // groups
    dma = pltpu.SemaphoreType.DMA
    smem = pl.BlockSpec(memory_space=pltpu.SMEM)
    vmem = pl.BlockSpec(memory_space=pltpu.VMEM)
    anywhere = pl.BlockSpec(memory_space=pl.ANY)
    block = pltpu.VMEM((shards,) + piece, BF16)
    return pl.pallas_call(
        functools.partial(merge_kernel, rows, by_columns),
        in_specs=[smem, smem, anywhere, vmem, vmem, anywhere, vmem, anywhere, vmem, anywhere],
        out_specs=[vmem, vmem],
        out_shape=[
            jax.ShapeDtypeStruct((tokens, feature), BF16),
            jax.ShapeDtypeStruct((1, seq), F32),
        ],
        scratch_shapes=[
            pltpu.VMEM((patch_rows, vit), BF16),
            pltpu.VMEM((per_token, tokens, vit), BF16),
            pltpu.VMEM((chunks, first_weight.shape[0], CHUNK), BF16),
            pltpu.VMEM((depth, width), BF16),
            pltpu.VMEM((seq, feature), BF16),
            pltpu.VMEM((rows, tokens), BF16),
            pltpu.VMEM((tokens, CHUNK), F32),
            pltpu.VMEM((shards, chunks, rows, CHUNK), BF16),
            pltpu.VMEM((shards, rows, width), BF16),
            pltpu.VMEM((shards, groups) + piece, BF16),
            pltpu.VMEM((shards, 2) + piece, BF16),
            block, block, block, block,
            pltpu.VMEM((1, seq), F32),
            pltpu.VMEM((groups, 1, seq), F32),
            dma((patch_rows // LANES,)), dma((chunks,)), dma, dma,
            dma((2, length, chunks)), dma((length, chunks)), dma((length, chunks)), dma((length, chunks)),
            dma((2, shards)), dma((2, shards)), dma((shards,)), dma((shards,)),
            dma((shards,)), dma((shards,)), dma((shards,)), dma((groups, per_group)),
            dma((groups - 1,)), dma((groups,)),
        ],
        compiler_params=pltpu.CompilerParams(
            collective_id=call_id, has_side_effects=True, vmem_limit_bytes=VMEM_LIMIT
        ),
        name="merge_%d" % rows,
    )(grids, routing, patches, norm_gain, norm_bias, first_weight, first_bias, second_weight, second_bias, text_embeds)


def scale_kernel(total_width, top_blocks, top_ref, text_ref, sums_ref, gain_ref, out_ref, normed_ref):
    rows = out_ref.shape[0]
    scale = lax.rsqrt(sums_ref[...] / total_width + 1e-06)
    scale = jnp.broadcast_to(scale, (LANES, rows)).T
    upper = pl.program_id(0) < top_blocks
    gain = gain_ref[...][None, :]
    for f in range(out_ref.shape[1] // LANES):
        span = slice(f * LANES, (f + 1) * LANES)
        values = jnp.where(upper, top_ref[:, span].astype(F32), text_ref[:, span].astype(F32))
        out_ref[:, span] = values.astype(BF16)
        normed_ref[:, span] = (values * scale * gain[:, span]).astype(BF16)


def scale_rows(top, text_embeds, sums, final_gain, groups):
    seq, feature = text_embeds.shape
    top_blocks = top.shape[0] // LANES
    block = pl.BlockSpec((LANES, feature), lambda i: (i, 0))
    return pl.pallas_call(
        functools.partial(scale_kernel, feature * groups, top_blocks),
        grid=(seq // LANES,),
        in_specs=[
            pl.BlockSpec((LANES, feature), lambda i: (jnp.minimum(i, top_blocks - 1), 0)),
            block,
            pl.BlockSpec((1, LANES), lambda i: (0, i)),
            pl.BlockSpec((feature,), lambda i: (0,)),
        ],
        out_specs=[block, block],
        out_shape=[jax.ShapeDtypeStruct((seq, feature), BF16)] * 2,
        compiler_params=pltpu.CompilerParams(vmem_limit_bytes=VMEM_LIMIT),
        name="scale_rows",
    )(top, text_embeds, sums, final_gain)


def bucket_sizes(slots, width, groups):
    step = slots // 16 if width % (groups * LANES) == 0 else slots // 4
    return tuple(b for b in range(slots // 2 + step, slots + 1, step) if b <= slots * 13 // 16 or b == slots)


def per_device(
    patches,
    norm_gain,
    norm_bias,
    first_weight,
    first_bias,
    second_weight,
    second_bias,
    text_embeds,
    final_gain,
    image_grids,
    routing,
):
    shards = lax.axis_size("dp")
    groups = lax.axis_size("tensor")
    slots = patches.shape[0] * patches.shape[1] // first_weight.shape[0]
    buckets = BUCKETS(slots, second_weight.shape[1], groups)
    smem = pl.BlockSpec(memory_space=pltpu.SMEM)
    which = pl.pallas_call(
        functools.partial(plan_kernel, buckets),
        in_specs=[smem, smem],
        out_specs=smem,
        out_shape=jax.ShapeDtypeStruct((1,), jnp.int32),
        name="plan",
    )(image_grids, routing)

    def branch(rows, call_id):
        return lambda: merge(
            rows, call_id, shards, groups, image_grids, routing, patches, norm_gain, norm_bias,
            first_weight, first_bias, second_weight, second_bias, text_embeds,
        )

    top, sums = lax.switch(which[0], [branch(rows, i) for i, rows in enumerate(buckets)])
    return tuple(scale_rows(top, text_embeds, sums, final_gain, groups))


BUCKETS = bucket_sizes


def solution(mesh):
    placed = (
        P("dp", None),
        P(),
        P(),
        P(None, "tensor"),
        P("tensor"),
        P("tensor", "dp"),
        P("tensor"),
        P("dp", "tensor"),
        P("tensor"),
        P(),
        P(),
    )
    return jax.shard_map(
        per_device,
        mesh=mesh,
        in_specs=placed,
        out_specs=(P("dp", "tensor"), P("dp", "tensor")),
        check_vma=False,
    )
```

```python
import functools

import jax
import jax.numpy as jnp
from jax import lax
from jax.experimental import pallas as pl
from jax.experimental.pallas import tpu as pltpu
from jax.sharding import PartitionSpec as P

VMEM_LIMIT = 62 * 1024 * 1024
LANES = 128
LN_GROUP = 128
CHUNK = 256
F32 = jnp.float32
BF16 = jnp.bfloat16


def area_of(grids_ref, s, b):
    return grids_ref[b, 0, s] * grids_ref[b, 1, s]


def segment(grids_ref, routing_ref, s, k):
    count, start = jnp.int32(0), jnp.int32(0)
    for b in range(routing_ref.shape[0]):
        area, offset = area_of(grids_ref, s, b), routing_ref[b, s]
        count = count + jnp.where(offset == k, area, 0)
        start = start + jnp.where(offset < k, area, 0)
    return count, start


def table_copies(grids_hbm, routing_hbm, grids_ref, routing_ref, table_sem):
    return (
        pltpu.make_async_copy(grids_hbm, grids_ref, table_sem.at[0]),
        pltpu.make_async_copy(routing_hbm, routing_ref, table_sem.at[1]),
    )


def plan_kernel(buckets, grids_hbm, routing_hbm, which_ref, grids_ref, routing_ref, table_sem):
    strides, shards = routing_ref.shape
    copies = table_copies(grids_hbm, routing_hbm, grids_ref, routing_ref, table_sem)
    for copy in copies:
        copy.start()
    for copy in copies:
        copy.wait()

    def widest(e, most):
        sent, filled = jnp.int32(0), jnp.int32(0)
        for k in range(strides):
            sent = sent + area_of(grids_ref, e, k)
            filled = filled + segment(grids_ref, routing_ref, (e + shards - k) % shards, k)[0]
        return jnp.maximum(most, jnp.maximum(sent, filled))

    most = lax.fori_loop(0, shards, widest, jnp.int32(0))
    which = jnp.int32(0)
    for bucket in buckets[:-1]:
        which = which + (most > bucket).astype(jnp.int32)
    which_ref[0] = which


def merge_kernel(
    rows, by_columns,
    grids_hbm, routing_hbm, patches_ref, gain_ref, bias_ref, first_ref, first_bias_ref, second_ref, second_bias_ref, text_ref,
    top_ref, sums_ref,
    grids_ref, routing_ref, out_ref, patch_buf, norm_a, norm_b, merged, first_buf, second_buf, text_buf, own_pick, acc, gath, sums, proj,
    part, pair_in, cross_out, cross_in, ready_buf, sums_out, sums_in,
    top_sem, table_sem, patch_sem, first_sem, second_sem, text_sem,
    line_send, line_recv, extra_send, extra_recv, pair_send, pair_recv, swap_send, swap_recv, cross_send, cross_recv,
    out_send, out_recv, sums_send, sums_recv,
):
    shards, chunks = gath.shape[0], gath.shape[1]
    strides = routing_ref.shape[0]
    groups, piece_rows, piece_cols = part.shape[1:]
    per_group = shards // groups
    length = shards // 2
    per_token, tokens, vit = merged.shape
    cap = tokens // strides
    depth, width = second_buf.shape
    cut = (chunks + 1) // 2
    ln_rows = LANES
    ln_steps = patch_buf.shape[0] // ln_rows
    ln_tokens = ln_rows // per_token
    seq = text_buf.shape[0]
    feature = text_buf.shape[1]
    top_rows = out_ref.shape[0]

    me = lax.axis_index("dp")
    group = lax.axis_index("tensor")
    place, row = me // 2, me % 2
    other = me + 1 - 2 * row
    core, side = group % 2, group // 2
    mate = 2 * side + 1 - core
    across = group + 2 - 4 * side
    across_mate = mate + 2 - 4 * side
    peers = (mate, across, across_mate)

    target = me // per_group
    barrier = pltpu.get_barrier_semaphore()
    pl.semaphore_signal(barrier, inc=1, device_id={"dp": other})
    for way, end in ((1, length - 1), (-1, 0)):

        @pl.when(place != end)
        def _(way=way):
            pl.semaphore_signal(barrier, inc=1, device_id={"dp": me + 2 * way})

    for peer in peers:
        pl.semaphore_signal(barrier, inc=1, device_id={"tensor": peer})

    def over_senders(body):
        def run(i, carry):
            sender, source = i % groups, group * per_group + i // groups

            @pl.when((sender != group) | (source != me))
            def _():
                body(source, sender)

            return carry

        lax.fori_loop(0, shards, run, 0)

    def greet(source, sender):
        pl.semaphore_signal(barrier, inc=1, device_id={"dp": source, "tensor": sender})

    over_senders(greet)
    near = 1 + (place > 0).astype(jnp.int32) + (place < length - 1).astype(jnp.int32)
    greeted = near + len(peers) + shards - (target == group).astype(jnp.int32)

    def patch_copy(i):
        span = pl.ds(pl.multiple_of(i * ln_rows, ln_rows), ln_rows)
        return pltpu.make_async_copy(patches_ref.at[span, :], patch_buf.at[span, :], patch_sem.at[i])

    def first_copy(c):
        span = pl.ds(pl.multiple_of(c * CHUNK, CHUNK), CHUNK)
        return pltpu.make_async_copy(first_ref.at[:, span], first_buf.at[c], first_sem.at[c])

    second_copy = pltpu.make_async_copy(second_ref, second_buf, second_sem)
    text_copy = pltpu.make_async_copy(text_ref, text_buf, text_sem)

    def start_patch(i, carry):
        patch_copy(i).start()
        return carry

    lax.fori_loop(0, ln_steps, start_patch, 0)
    tables = table_copies(grids_hbm, routing_hbm, grids_ref, routing_ref, table_sem)
    for table in tables:
        table.start()

    gain = gain_ref[...][None, :]
    bias = bias_ref[...][None, :]
    line = lax.broadcasted_iota(jnp.int32, (ln_rows, ln_rows), 0)
    wanted = per_token * (line % ln_tokens) + line // ln_tokens
    regroup = (lax.broadcasted_iota(jnp.int32, (ln_rows, ln_rows), 1) == wanted).astype(F32).astype(BF16)

    def norm_rows(i, norm_buf):
        patch_copy(i).wait()
        for r in range(0, ln_rows, LN_GROUP):
            values = patch_buf[pl.ds(pl.multiple_of(i * ln_rows + r, LN_GROUP), LN_GROUP), :].astype(F32)
            centered = values - jnp.mean(values, axis=-1, keepdims=True)
            variance = jnp.mean(centered * centered, axis=-1, keepdims=True)
            norm_buf[r:r + LN_GROUP] = (centered * lax.rsqrt(variance + 1e-06) * gain + bias).astype(BF16)

    def merge_rows(i, norm_buf):
        sorted_rows = jnp.dot(regroup, norm_buf[...], preferred_element_type=F32).astype(BF16)
        for j in range(per_token):
            merged[j, pl.ds(pl.multiple_of(i * ln_tokens, ln_tokens), ln_tokens), :] = sorted_rows[j * ln_tokens:(j + 1) * ln_tokens]

    def norm_pair(h, carry):
        for i in (2 * h, 2 * h + 1):

            @pl.when(i < chunks)
            def _(i=i):
                first_copy(i).start()

        @pl.when(h == ln_steps // 2 - 1)
        def _():
            second_copy.start()
            text_copy.start()

        norm_rows(2 * h, norm_a)
        norm_rows(2 * h + 1, norm_b)
        merge_rows(2 * h, norm_a)
        merge_rows(2 * h + 1, norm_b)
        return carry

    lax.fori_loop(0, ln_steps // 2, norm_pair, 0)
    for table in tables:
        table.wait()

    token_row = lax.broadcasted_iota(jnp.int32, (rows, tokens), 0)
    token_gap = lax.broadcasted_iota(jnp.int32, (rows, tokens), 1) - token_row
    picked = jnp.zeros((rows, tokens), jnp.bool_)
    for b in range(strides):
        offset = routing_ref[b, me]
        start = jnp.int32(0)
        for o in range(strides):
            start = start + jnp.where(routing_ref[o, me] < offset, area_of(grids_ref, me, o), 0)
        stop = start + area_of(grids_ref, me, b)
        picked = picked | ((token_row >= start) & (token_row < stop) & (token_gap == b * cap - start))
    own_pick[...] = picked.astype(F32).astype(BF16)

    pl.semaphore_wait(barrier, greeted)

    def hidden_chunk(c):
        first_copy(c).wait()

        def add(j, carry):
            weight = first_buf[c, pl.ds(pl.multiple_of(j * vit, vit), vit), :]
            term = jnp.dot(merged[j], weight, preferred_element_type=F32)
            acc[...] = jnp.where(j == 0, term, acc[...] + term)
            return carry

        lax.fori_loop(0, per_token, add, 0)
        x = acc[...] + first_bias_ref[pl.ds(pl.multiple_of(c * CHUNK, CHUNK), CHUNK)][None, :]
        hidden = (0.5 * x * (1.0 + lax.erf(x * (0.5 ** 0.5)))).astype(BF16)
        gath[me, c] = jnp.dot(own_pick[...], hidden, preferred_element_type=F32).astype(BF16)

    def line_copy(block, c, way):
        here = gath.at[2 * block + row, c]
        return pltpu.make_async_remote_copy(
            src_ref=here,
            dst_ref=here,
            send_sem=line_send.at[(way + 1) // 2, block, c],
            recv_sem=line_recv.at[block, c],
            device_id={"dp": me + 2 * way},
        )

    def by_line(block, c):
        first, last = (block == 0) & (place != 0), (block == length - 1) & (place != length - 1)
        return (c >= cut) & (first | last)

    def extra_copy(c, way):
        here = gath.at[(length - 1) * (1 - way) + 1 - row, c]
        return pltpu.make_async_remote_copy(
            src_ref=here,
            dst_ref=here,
            send_sem=extra_send.at[(way + 1) // 2, c],
            recv_sem=extra_recv.at[(way + 1) // 2, c],
            device_id={"dp": me + 2 * way},
        )

    def pair_copy(block, c, side_row):
        here = gath.at[2 * block + side_row, c]
        return pltpu.make_async_remote_copy(
            src_ref=here,
            dst_ref=here,
            send_sem=pair_send.at[block, c],
            recv_sem=pair_recv.at[block, c],
            device_id={"dp": other},
        )

    def swap_copy(e, slot):
        return pltpu.make_async_remote_copy(
            src_ref=part.at[e, mate if slot == 0 else across_mate],
            dst_ref=pair_in.at[e, slot],
            send_sem=swap_send.at[slot, e],
            recv_sem=swap_recv.at[slot, e],
            device_id={"tensor": mate},
        )

    def cross_copy(e):
        return pltpu.make_async_remote_copy(
            src_ref=cross_out.at[e],
            dst_ref=cross_in.at[e],
            send_sem=cross_send.at[e],
            recv_sem=cross_recv.at[e],
            device_id={"tensor": across},
        )

    def place_of(source, sender):
        if by_columns:
            at = ((source % per_group) * groups + sender) * piece_cols
            return pl.ds(0, rows), pl.ds(pl.multiple_of(at, piece_cols), piece_cols)
        return (
            pl.ds(pl.multiple_of(sender * piece_rows, piece_rows), piece_rows),
            pl.ds(pl.multiple_of((source % per_group) * piece_cols, piece_cols), piece_cols),
        )

    def out_copy(e, source, sender):
        return pltpu.make_async_remote_copy(
            src_ref=ready_buf.at[e],
            dst_ref=out_ref.at[place_of(source, sender)],
            send_sem=out_send.at[e],
            recv_sem=out_recv.at[sender, source % per_group],
            device_id={"dp": e, "tensor": target},
        )

    def compute_ready(e):
        last = jnp.int32(0)
        for k in range(strides):
            source = (e + shards - k) % shards
            away = jnp.abs(source // 2 - place) + jnp.abs(source % 2 - row)
            last = jnp.maximum(last, away)
        return last

    packed = jnp.int32(0)
    if shards <= 8:
        for e in range(shards):
            packed = packed + compute_ready(jnp.int32(e)) * (1 << (3 * e))

    def ready_step(e):
        return (packed >> (3 * e)) & 7 if shards <= 8 else compute_ready(e)

    def over_shards(body):
        def run(i, carry):
            body((me + 1 + i) % shards)
            return carry

        lax.fori_loop(0, shards, run, 0)

    def accumulate(source, c, way, kind):
        slot = 2 * kind + (way + 1) // 2
        weight = second_buf[pl.ds(pl.multiple_of(c * CHUNK, CHUNK), CHUNK), :]
        term = jnp.dot(gath[source, c], weight, preferred_element_type=F32)
        sums[slot] = jnp.where(c == 0, term, sums[slot] + term)

    def pick(e):
        at_row = lax.broadcasted_iota(jnp.int32, (rows, rows), 0)
        gap = lax.broadcasted_iota(jnp.int32, (rows, rows), 1) - at_row
        laid = jnp.int32(0)
        total = None
        for k in range(strides):
            source = (e + shards - k) % shards
            count, start = segment(grids_ref, routing_ref, source, k)
            chosen = (at_row >= laid) & (at_row < laid + count) & (gap == start - laid)
            term = jnp.dot(chosen.astype(F32).astype(BF16), proj[source], preferred_element_type=F32)
            total = term if total is None else total + term
            laid = laid + count
        total = total.astype(BF16)
        for g in range(groups):
            if by_columns:
                part[e, g] = total[:, g * piece_cols:(g + 1) * piece_cols]
            else:
                part[e, g] = total[g * piece_rows:(g + 1) * piece_rows]
        for slot in (1, 0):
            swap_copy(e, slot).start()

    def cross(e):
        swap_copy(e, 1).wait_recv()
        cross_out[e] = (part[e, across].astype(F32) + pair_in[e, 1].astype(F32)).astype(BF16)
        cross_copy(e).start()

    def finish(e):
        swap_copy(e, 0).wait_recv()
        cross_copy(e).wait_recv()
        total = (part[e, group].astype(F32) + pair_in[e, 0].astype(F32) + cross_in[e].astype(F32)).astype(BF16)

        stays = (e == me) & (target == group)

        @pl.when(jnp.logical_not(stays))
        def _():
            ready_buf[e] = total
            out_copy(e, me, group).start()

        @pl.when(stays)
        def _():
            at_rows, at_cols = place_of(me, group)
            out_ref[at_rows, at_cols] = total

    def row_sums(values):
        squares = values * values
        lanes = squares[:, :LANES]
        for f in range(1, feature // LANES):
            lanes = lanes + squares[:, f * LANES:(f + 1) * LANES]
        return jnp.sum(lanes.T, axis=0, keepdims=True)

    def text_sums():
        text_copy.wait()

        def block(i, carry):
            span = pl.ds(pl.multiple_of(i * LANES, LANES), LANES)
            sums_out[:, span] = row_sums(text_buf[span, :].astype(F32))
            return carry

        lax.fori_loop(0, seq // LANES, block, 0)

    def is_block(block, away, way):
        return (away >= 0) & (away < length) & ((away > 0) | (way == 1)) & (block >= 0) & (block < length)

    def slot_step(step, c):
        @pl.when(step == 0)
        def _():
            hidden_chunk(c)

        for way in (1, -1):
            block = place - way * step
            have = (step < length) & (block >= 0) & (block < length)

            @pl.when(have & (step > 0))
            def _(block=block, way=way):
                line_copy(block, c, way).wait_recv()

            @pl.when(have & (place + way >= 0) & (place + way < length))
            def _(block=block, way=way):
                line_copy(block, c, way).start()

            @pl.when(is_block(block, step, way) & jnp.logical_not(by_line(block, c)))
            def _(block=block):
                pair_copy(block, c, row).start()

        for way in (1, -1):
            away = place if way == 1 else length - 1 - place

            @pl.when((away > 0) & (step == away + 1) & (c < chunks - cut))
            def _(away=away, way=way):
                extra_copy(c + cut, way).wait_recv()

                @pl.when(away < length - 1)
                def _():
                    extra_copy(c + cut, way).start()

        @pl.when((step == 0) & (c == 0))
        def _():
            second_copy.wait()

        @pl.when((step == 1) & (c == 3))
        def _():
            text_sums()

        @pl.when((step > 0) & (c > 0) & (c < 3))
        def _():
            def now(e):
                @pl.when((ready_step(e) == step - 1) & (e % 2 == c - 1))
                def _():
                    cross(e)

            over_shards(now)

        @pl.when((step > 0) & (c < 2))
        def _():
            def now(e):
                @pl.when((ready_step(e) == step - 1) & (e % 2 == c))
                def _():
                    pick(e)

            over_shards(now)

        @pl.when((step == length) & (c == 3))
        def _():
            def now(e):
                @pl.when(ready_step(e) <= length - 2)
                def _():
                    finish(e)

            over_shards(now)

        def unit(i, carry):
            way = 1 - 2 * (i % 2)
            block = place - way * step

            @pl.when(is_block(block, step, way))
            def _():
                accumulate(2 * block + row, c, way, 0)

            return carry

        lax.fori_loop(0, 2, unit, 0)

        def other_unit(i, carry):
            way = 1 - 2 * (i % 2)
            block = place - way * (step - 1)
            far = i // 2
            plain = is_block(block, step - 1, way)
            split = ((block == 0) & (place != 0)) | ((block == length - 1) & (place != length - 1))
            near = (far == 0) & plain & jnp.logical_not((c >= cut) & split)

            @pl.when(near)
            def _():
                pair_copy(block, c, 1 - row).wait_recv()

            @pl.when(near | ((far == 1) & plain & split & (c < chunks - cut)))
            def _():
                accumulate(2 * block + 1 - row, c + far * cut, way, 1)

            return carry

        lax.fori_loop(0, 4, other_unit, 0)

        for way, end in ((1, 0), (-1, length - 1)):

            @pl.when((step == 1) & (c >= cut) & (place == end))
            def _(way=way):
                extra_copy(c, way).start()

        @pl.when(c == chunks - 1)
        def _():
            def settle_unit(i, carry):
                way, kind = 1 - 2 * (i % 2), i // 2
                block = place - way * (step - kind)

                @pl.when(is_block(block, step - kind, way))
                def _():
                    source = 2 * block + jnp.abs(row - kind)
                    proj[source] = sums[2 * kind + (way + 1) // 2].astype(BF16)

                return carry

            lax.fori_loop(0, 4, settle_unit, 0)

    def outer(step, carry):
        def inner(c, carry):
            slot_step(step, c)
            return carry

        return lax.fori_loop(0, chunks, inner, carry)

    steps = length + 1 + ((place == 0) | (place == length - 1)).astype(jnp.int32)
    lax.fori_loop(0, steps, outer, 0)

    for step in (length - 1, length):

        def now(e, step=step):
            @pl.when(ready_step(e) == step)
            def _():
                finish(e)

        over_shards(now)

    def arrive(source, sender):
        out_copy(me, source, sender).wait_recv()

    over_senders(arrive)

    filled = jnp.int32(0)
    for k in range(strides):
        filled = filled + segment(grids_ref, routing_ref, (me + shards - k) % shards, k)[0]

    second_bias = second_bias_ref[...][None, :]
    if rows < top_rows:
        out_ref[rows:, :] = text_buf[rows:top_rows, :]

    def splice(i, carry):
        span = pl.ds(pl.multiple_of(i * LANES, LANES), LANES)
        image = (out_ref[span, :].astype(F32) + second_bias).astype(BF16)
        line = lax.broadcasted_iota(jnp.int32, (LANES, feature), 0) + i * LANES
        values = jnp.where(line < filled, image.astype(F32), text_buf[span, :].astype(F32))
        out_ref[span, :] = values.astype(BF16)
        sums_out[:, span] = row_sums(values)
        return carry

    lax.fori_loop(0, top_rows // LANES, splice, 0)
    top_copy = pltpu.make_async_copy(out_ref, top_ref, top_sem)

    def sums_copy(peer, sender, i):
        return pltpu.make_async_remote_copy(
            src_ref=sums_out,
            dst_ref=sums_in.at[sender],
            send_sem=sums_send.at[i],
            recv_sem=sums_recv.at[sender],
            device_id={"tensor": peer},
        )

    for i, peer in enumerate(peers):
        sums_copy(peer, group, i).start()
    top_copy.start()

    def drain_line(t, carry):
        block, c = t // chunks, t % chunks

        @pl.when(jnp.logical_not(by_line(block, c)))
        def _():
            pair_copy(block, c, row).wait_send()

        @pl.when((block <= place) & (place < length - 1))
        def _():
            line_copy(block, c, 1).wait_send()

        @pl.when((block >= place) & (place > 0))
        def _():
            line_copy(block, c, -1).wait_send()

        return carry

    lax.fori_loop(0, length * chunks, drain_line, 0)

    def drain_extra(c, carry):
        for way, end in ((1, length - 1), (-1, 0)):

            @pl.when(place != end)
            def _(way=way):
                extra_copy(c, way).wait_send()

        return carry

    lax.fori_loop(cut, chunks, drain_extra, 0)

    def drain(e):
        for slot in (1, 0):
            swap_copy(e, slot).wait_send()
        cross_copy(e).wait_send()

        @pl.when((e != me) | (target != group))
        def _():
            out_copy(e, me, group).wait_send()

    over_shards(drain)
    total = sums_out[...]
    for i, peer in enumerate(peers):
        copy = sums_copy(peer, peer, i)
        copy.wait_recv()
        copy.wait_send()
        total = total + sums_in[peer]
    sums_ref[...] = total
    top_copy.wait()


def merge(rows, call_id, shards, groups, grids, routing, patches, norm_gain, norm_bias, first_weight, first_bias, second_weight, second_bias, text_embeds):
    patch_rows, vit = patches.shape
    per_token = first_weight.shape[0] // vit
    tokens = patch_rows // per_token
    hidden_width = first_weight.shape[1]
    chunks = hidden_width // CHUNK
    depth, width = second_weight.shape
    seq, feature = text_embeds.shape
    length = shards // 2
    by_columns = width % (groups * LANES) == 0
    piece = (rows, width // groups) if by_columns else (rows // groups, width)
    per_group = shards // groups
    dma = pltpu.SemaphoreType.DMA
    vmem = pl.BlockSpec(memory_space=pltpu.VMEM)
    anywhere = pl.BlockSpec(memory_space=pl.ANY)
    block = pltpu.VMEM((shards,) + piece, BF16)
    return pl.pallas_call(
        functools.partial(merge_kernel, rows, by_columns),
        in_specs=[anywhere, anywhere, anywhere, vmem, vmem, anywhere, vmem, anywhere, vmem, anywhere],
        out_specs=[anywhere, vmem],
        out_shape=[
            jax.ShapeDtypeStruct((tokens, feature), BF16),
            jax.ShapeDtypeStruct((1, seq), F32),
        ],
        scratch_shapes=[
            pltpu.SMEM(grids.shape, jnp.int32),
            pltpu.SMEM(routing.shape, jnp.int32),
            pltpu.VMEM((tokens, feature), BF16),
            pltpu.VMEM((patch_rows, vit), BF16),
            pltpu.VMEM((LANES, vit), BF16),
            pltpu.VMEM((LANES, vit), BF16),
            pltpu.VMEM((per_token, tokens, vit), BF16),
            pltpu.VMEM((chunks, first_weight.shape[0], CHUNK), BF16),
            pltpu.VMEM((depth, width), BF16),
            pltpu.VMEM((seq, feature), BF16),
            pltpu.VMEM((rows, tokens), BF16),
            pltpu.VMEM((tokens, CHUNK), F32),
            pltpu.VMEM((shards, chunks, rows, CHUNK), BF16),
            pltpu.VMEM((4, rows, width), F32),
            pltpu.VMEM((shards, rows, width), BF16),
            pltpu.VMEM((shards, groups) + piece, BF16),
            pltpu.VMEM((shards, 2) + piece, BF16),
            block, block, block,
            pltpu.VMEM((1, seq), F32),
            pltpu.VMEM((groups, 1, seq), F32),
            dma, dma((2,)), dma((patch_rows // LANES,)), dma((chunks,)), dma, dma,
            dma((2, length, chunks)), dma((length, chunks)), dma((2, chunks)), dma((2, chunks)),
            dma((length, chunks)), dma((length, chunks)),
            dma((2, shards)), dma((2, shards)), dma((shards,)), dma((shards,)),
            dma((shards,)), dma((groups, per_group)),
            dma((groups - 1,)), dma((groups,)),
        ],
        compiler_params=pltpu.CompilerParams(
            collective_id=call_id, has_side_effects=True, vmem_limit_bytes=VMEM_LIMIT
        ),
        name="merge_%d" % rows,
    )(grids, routing, patches, norm_gain, norm_bias, first_weight, first_bias, second_weight, second_bias, text_embeds)


def scale_kernel(total_width, top_ref, text_ref, sums_ref, gain_ref, out_ref, normed_ref, rows_buf, normed_buf, in_sem, out_sem, normed_sem):
    feature = gain_ref.shape[0]
    blocks, top_blocks = rows_buf.shape[0], top_ref.shape[0] // LANES

    def in_copy(i):
        source = top_ref if i < top_blocks else text_ref
        return pltpu.make_async_copy(source.at[pl.ds(i * LANES, LANES)], rows_buf.at[i], in_sem.at[i])

    def span_of(i):
        return pl.ds(pl.multiple_of(i * LANES, LANES), LANES)

    def out_copy(i):
        return pltpu.make_async_copy(rows_buf.at[i], out_ref.at[span_of(i)], out_sem.at[i])

    def normed_copy(i):
        return pltpu.make_async_copy(normed_buf.at[i], normed_ref.at[span_of(i)], normed_sem.at[i])

    for i in range(blocks):
        in_copy(i).start()
    gain = gain_ref[...][None, :]

    for i in range(blocks):
        in_copy(i).wait()
        out_copy(i).start()
        scale = lax.rsqrt(sums_ref[:, pl.ds(i * LANES, LANES)] / total_width + 1e-06)
        scale = jnp.broadcast_to(scale, (LANES, LANES)).T
        for f in range(feature // LANES):
            span = slice(f * LANES, (f + 1) * LANES)
            normed_buf[i, :, span] = (rows_buf[i, :, span].astype(F32) * scale * gain[:, span]).astype(BF16)
        normed_copy(i).start()

    for i in range(blocks):
        out_copy(i).wait()
        normed_copy(i).wait()


def scale_rows(top, text_embeds, sums, final_gain, groups):
    seq, feature = text_embeds.shape
    anywhere = pl.BlockSpec(memory_space=pl.ANY)
    vmem = pl.BlockSpec(memory_space=pltpu.VMEM)
    blocks = seq // LANES
    dma = pltpu.SemaphoreType.DMA
    return pl.pallas_call(
        functools.partial(scale_kernel, feature * groups),
        in_specs=[anywhere, anywhere, vmem, vmem],
        out_specs=[anywhere, anywhere],
        out_shape=[jax.ShapeDtypeStruct((seq, feature), BF16)] * 2,
        scratch_shapes=[
            pltpu.VMEM((blocks, LANES, feature), BF16),
            pltpu.VMEM((blocks, LANES, feature), BF16),
            dma((blocks,)), dma((blocks,)), dma((blocks,)),
        ],
        compiler_params=pltpu.CompilerParams(vmem_limit_bytes=VMEM_LIMIT),
        name="scale_rows",
    )(top, text_embeds, sums, final_gain)


def bucket_sizes(slots, width, groups):
    step = slots // 16 if width % (groups * LANES) == 0 else slots // 4
    return tuple(b for b in range(slots // 2 + step, slots + 1, step) if b <= slots * 13 // 16 or b == slots)


def per_device(
    patches,
    norm_gain,
    norm_bias,
    first_weight,
    first_bias,
    second_weight,
    second_bias,
    text_embeds,
    final_gain,
    image_grids,
    routing,
):
    shards = lax.axis_size("dp")
    groups = lax.axis_size("tensor")
    slots = patches.shape[0] * patches.shape[1] // first_weight.shape[0]
    grids, offsets = image_grids.transpose(1, 2, 0), routing.T
    buckets = BUCKETS(slots, second_weight.shape[1], groups)
    which = pl.pallas_call(
        functools.partial(plan_kernel, buckets),
        in_specs=[pl.BlockSpec(memory_space=pl.ANY)] * 2,
        out_specs=pl.BlockSpec(memory_space=pltpu.SMEM),
        out_shape=jax.ShapeDtypeStruct((1,), jnp.int32),
        scratch_shapes=[
            pltpu.SMEM(grids.shape, jnp.int32),
            pltpu.SMEM(offsets.shape, jnp.int32),
            pltpu.SemaphoreType.DMA((2,)),
        ],
        name="plan",
    )(grids, offsets)

    def branch(rows, call_id):
        return lambda: merge(
            rows, call_id, shards, groups, grids, offsets, patches, norm_gain, norm_bias,
            first_weight, first_bias, second_weight, second_bias, text_embeds,
        )

    top, sums = lax.switch(which[0], [branch(rows, i) for i, rows in enumerate(buckets)])
    return tuple(scale_rows(top, text_embeds, sums, final_gain, groups))


BUCKETS = bucket_sizes


def solution(mesh):
    placed = (
        P("dp", None),
        P(),
        P(),
        P(None, "tensor"),
        P("tensor"),
        P("tensor", "dp"),
        P("tensor"),
        P("dp", "tensor"),
        P("tensor"),
        P(),
        P(),
    )
    return jax.shard_map(
        per_device,
        mesh=mesh,
        in_specs=placed,
        out_specs=(P("dp", "tensor"), P("dp", "tensor")),
        check_vma=False,
    )
```

```python
import functools

import jax
import jax.numpy as jnp
from jax import lax
from jax.experimental import pallas as pl
from jax.experimental.pallas import tpu as pltpu
from jax.sharding import PartitionSpec as P

VMEM_LIMIT = 62 * 1024 * 1024
LANES = 128
LN_GROUP = 128
CHUNK = 256
F32 = jnp.float32
BF16 = jnp.bfloat16


def area_of(grids_ref, s, b):
    return grids_ref[b, 0, s] * grids_ref[b, 1, s]


def segment(grids_ref, routing_ref, s, k):
    count, start = jnp.int32(0), jnp.int32(0)
    for b in range(routing_ref.shape[0]):
        area, offset = area_of(grids_ref, s, b), routing_ref[b, s]
        count = count + jnp.where(offset == k, area, 0)
        start = start + jnp.where(offset < k, area, 0)
    return count, start


def table_copies(grids_hbm, routing_hbm, grids_ref, routing_ref, table_sem):
    return (
        pltpu.make_async_copy(grids_hbm, grids_ref, table_sem.at[0]),
        pltpu.make_async_copy(routing_hbm, routing_ref, table_sem.at[1]),
    )


def plan_kernel(buckets, grids_hbm, routing_hbm, which_ref, grids_ref, routing_ref, filled_ref, table_sem):
    strides, shards = routing_ref.shape
    copies = table_copies(grids_hbm, routing_hbm, grids_ref, routing_ref, table_sem)
    for copy in copies:
        copy.start()
    for copy in copies:
        copy.wait()

    for e in range(shards):
        filled_ref[e] = 0
    most = jnp.int32(0)
    for s in range(shards):
        sent = jnp.int32(0)
        for b in range(strides):
            area = area_of(grids_ref, s, b)
            sent = sent + area
            e = s + routing_ref[b, s]
            e = jnp.where(e >= shards, e - shards, e)
            filled_ref[e] = filled_ref[e] + area
        most = jnp.maximum(most, sent)
    for e in range(shards):
        most = jnp.maximum(most, filled_ref[e])
    which = jnp.int32(0)
    for bucket in buckets[:-1]:
        which = which + (most > bucket).astype(jnp.int32)
    which_ref[0] = which


def merge_kernel(
    rows, by_columns,
    grids_hbm, routing_hbm, patches_ref, gain_ref, bias_ref, first_ref, first_bias_ref, second_ref, second_bias_ref, text_ref,
    top_ref, sums_ref,
    grids_ref, routing_ref, lane_sums, out_ref, patch_buf, norm_a, norm_b, merged, first_buf, second_buf, text_buf, own_pick, acc, gath, sums, proj,
    part, pair_in, cross_out, cross_in, ready_buf, sums_out, sums_in,
    top_sem, table_sem, patch_sem, first_sem, second_sem, text_sem,
    line_send, line_recv, extra_send, extra_recv, pair_send, pair_recv, swap_send, swap_recv, cross_send, cross_recv,
    out_send, out_recv, sums_send, sums_recv,
):
    shards, chunks = gath.shape[0], gath.shape[1]
    strides = routing_ref.shape[0]
    groups, piece_rows, piece_cols = part.shape[1:]
    per_group = shards // groups
    length = shards // 2
    per_token, tokens, vit = merged.shape
    cap = tokens // strides
    depth, width = second_buf.shape
    cut = (chunks + 1) // 2
    ln_rows = LANES
    ln_steps = patch_buf.shape[0] // ln_rows
    ln_tokens = ln_rows // per_token
    seq = text_buf.shape[0]
    feature = text_buf.shape[1]
    top_rows = out_ref.shape[0]

    me = lax.axis_index("dp")
    group = lax.axis_index("tensor")
    place, row = me // 2, me % 2
    other = me + 1 - 2 * row
    core, side = group % 2, group // 2
    mate = 2 * side + 1 - core
    across = group + 2 - 4 * side
    across_mate = mate + 2 - 4 * side
    peers = (mate, across, across_mate)

    target = me // per_group
    barrier = pltpu.get_barrier_semaphore()
    pl.semaphore_signal(barrier, inc=1, device_id={"dp": other})
    for way, end in ((1, length - 1), (-1, 0)):

        @pl.when(place != end)
        def _(way=way):
            pl.semaphore_signal(barrier, inc=1, device_id={"dp": me + 2 * way})

    for peer in peers:
        pl.semaphore_signal(barrier, inc=1, device_id={"tensor": peer})

    def over_senders(body):
        def run(i, carry):
            sender, source = i % groups, group * per_group + i // groups

            @pl.when((sender != group) | (source != me))
            def _():
                body(source, sender)

            return carry

        lax.fori_loop(0, shards, run, 0)

    def greet(source, sender):
        pl.semaphore_signal(barrier, inc=1, device_id={"dp": source, "tensor": sender})

    over_senders(greet)
    near = 1 + (place > 0).astype(jnp.int32) + (place < length - 1).astype(jnp.int32)
    greeted = near + len(peers) + shards - (target == group).astype(jnp.int32)

    def patch_copy(i):
        span = pl.ds(pl.multiple_of(i * ln_rows, ln_rows), ln_rows)
        return pltpu.make_async_copy(patches_ref.at[span, :], patch_buf.at[span, :], patch_sem.at[i])

    def first_copy(c):
        span = pl.ds(pl.multiple_of(c * CHUNK, CHUNK), CHUNK)
        return pltpu.make_async_copy(first_ref.at[:, span], first_buf.at[c], first_sem.at[c])

    second_copy = pltpu.make_async_copy(second_ref, second_buf, second_sem)
    text_copy = pltpu.make_async_copy(text_ref, text_buf, text_sem)

    def start_patch(i, carry):
        patch_copy(i).start()
        return carry

    lax.fori_loop(0, ln_steps, start_patch, 0)
    tables = table_copies(grids_hbm, routing_hbm, grids_ref, routing_ref, table_sem)
    for table in tables:
        table.start()

    gain = gain_ref[...][None, :]
    bias = bias_ref[...][None, :]
    line = lax.broadcasted_iota(jnp.int32, (ln_rows, ln_rows), 0)
    wanted = per_token * (line % ln_tokens) + line // ln_tokens
    regroup = (lax.broadcasted_iota(jnp.int32, (ln_rows, ln_rows), 1) == wanted).astype(F32).astype(BF16)

    def norm_rows(i, norm_buf):
        patch_copy(i).wait()
        for r in range(0, ln_rows, LN_GROUP):
            values = patch_buf[pl.ds(pl.multiple_of(i * ln_rows + r, LN_GROUP), LN_GROUP), :].astype(F32)
            centered = values - jnp.mean(values, axis=-1, keepdims=True)
            variance = jnp.mean(centered * centered, axis=-1, keepdims=True)
            norm_buf[r:r + LN_GROUP] = (centered * lax.rsqrt(variance + 1e-06) * gain + bias).astype(BF16)

    def merge_rows(i, norm_buf):
        sorted_rows = jnp.dot(regroup, norm_buf[...], preferred_element_type=F32).astype(BF16)
        for j in range(per_token):
            merged[j, pl.ds(pl.multiple_of(i * ln_tokens, ln_tokens), ln_tokens), :] = sorted_rows[j * ln_tokens:(j + 1) * ln_tokens]

    def norm_pair(h, carry):
        for i in (2 * h, 2 * h + 1):

            @pl.when(i < chunks)
            def _(i=i):
                first_copy(i).start()

        @pl.when(h == ln_steps // 2 - 1)
        def _():
            second_copy.start()
            text_copy.start()

        norm_rows(2 * h, norm_a)
        norm_rows(2 * h + 1, norm_b)
        merge_rows(2 * h, norm_a)
        merge_rows(2 * h + 1, norm_b)
        return carry

    lax.fori_loop(0, ln_steps // 2, norm_pair, 0)
    for table in tables:
        table.wait()

    token_row = lax.broadcasted_iota(jnp.int32, (rows, tokens), 0)
    token_gap = lax.broadcasted_iota(jnp.int32, (rows, tokens), 1) - token_row
    picked = jnp.zeros((rows, tokens), jnp.bool_)
    for b in range(strides):
        offset = routing_ref[b, me]
        start = jnp.int32(0)
        for o in range(strides):
            start = start + jnp.where(routing_ref[o, me] < offset, area_of(grids_ref, me, o), 0)
        stop = start + area_of(grids_ref, me, b)
        picked = picked | ((token_row >= start) & (token_row < stop) & (token_gap == b * cap - start))
    own_pick[...] = picked.astype(F32).astype(BF16)

    pl.semaphore_wait(barrier, greeted)

    def hidden_chunk(c):
        first_copy(c).wait()

        def add(j, carry):
            weight = first_buf[c, pl.ds(pl.multiple_of(j * vit, vit), vit), :]
            term = jnp.dot(merged[j], weight, preferred_element_type=F32)
            acc[...] = jnp.where(j == 0, term, acc[...] + term)
            return carry

        lax.fori_loop(0, per_token, add, 0)
        x = acc[...] + first_bias_ref[pl.ds(pl.multiple_of(c * CHUNK, CHUNK), CHUNK)][None, :]
        hidden = (0.5 * x * (1.0 + lax.erf(x * (0.5 ** 0.5)))).astype(BF16)
        gath[me, c] = jnp.dot(own_pick[...], hidden, preferred_element_type=F32).astype(BF16)

    def line_copy(block, c, way):
        here = gath.at[2 * block + row, c]
        return pltpu.make_async_remote_copy(
            src_ref=here,
            dst_ref=here,
            send_sem=line_send.at[(way + 1) // 2, block, c],
            recv_sem=line_recv.at[block, c],
            device_id={"dp": me + 2 * way},
        )

    def by_line(block, c):
        first = (block == 0) & (place != 0) & ((c >= cut) | (place == 1))
        last = (block == length - 1) & (place != length - 1) & ((c >= cut) | (place == length - 2))
        return first | last

    def extra_copy(c, way):
        here = gath.at[(length - 1) * (1 - way) + 1 - row, c]
        return pltpu.make_async_remote_copy(
            src_ref=here,
            dst_ref=here,
            send_sem=extra_send.at[(way + 1) // 2, c],
            recv_sem=extra_recv.at[(way + 1) // 2, c],
            device_id={"dp": me + 2 * way},
        )

    def pair_copy(block, c, side_row):
        here = gath.at[2 * block + side_row, c]
        return pltpu.make_async_remote_copy(
            src_ref=here,
            dst_ref=here,
            send_sem=pair_send.at[block, c],
            recv_sem=pair_recv.at[block, c],
            device_id={"dp": other},
        )

    def swap_copy(e, slot):
        return pltpu.make_async_remote_copy(
            src_ref=part.at[e, mate if slot == 0 else across_mate],
            dst_ref=pair_in.at[e, slot],
            send_sem=swap_send.at[slot, e],
            recv_sem=swap_recv.at[slot, e],
            device_id={"tensor": mate},
        )

    def cross_copy(e):
        return pltpu.make_async_remote_copy(
            src_ref=cross_out.at[e],
            dst_ref=cross_in.at[e],
            send_sem=cross_send.at[e],
            recv_sem=cross_recv.at[e],
            device_id={"tensor": across},
        )

    def place_of(source, sender):
        if by_columns:
            at = ((source % per_group) * groups + sender) * piece_cols
            return pl.ds(0, rows), pl.ds(pl.multiple_of(at, piece_cols), piece_cols)
        return (
            pl.ds(pl.multiple_of(sender * piece_rows, piece_rows), piece_rows),
            pl.ds(pl.multiple_of((source % per_group) * piece_cols, piece_cols), piece_cols),
        )

    def out_copy(e, source, sender):
        return pltpu.make_async_remote_copy(
            src_ref=ready_buf.at[e],
            dst_ref=out_ref.at[place_of(source, sender)],
            send_sem=out_send.at[e],
            recv_sem=out_recv.at[sender, source % per_group],
            device_id={"dp": e, "tensor": target},
        )

    def compute_ready(e):
        last = jnp.int32(0)
        for k in range(strides):
            source = (e + shards - k) % shards
            away = jnp.abs(source // 2 - place) + jnp.abs(source % 2 - row)
            last = jnp.maximum(last, away)
        return last

    packed = jnp.int32(0)
    if shards <= 8:
        for e in range(shards):
            packed = packed + compute_ready(jnp.int32(e)) * (1 << (3 * e))

    def ready_step(e):
        return (packed >> (3 * e)) & 7 if shards <= 8 else compute_ready(e)

    def over_shards(body):
        def run(i, carry):
            body((me + 1 + i) % shards)
            return carry

        lax.fori_loop(0, shards, run, 0)

    def accumulate(source, c, slot):
        weight = second_buf[pl.ds(pl.multiple_of(c * CHUNK, CHUNK), CHUNK), :]
        term = jnp.dot(gath[source, c], weight, preferred_element_type=F32)
        sums[slot] = jnp.where(c == 0, term, sums[slot] + term)

    def pick(e):
        at_row = lax.broadcasted_iota(jnp.int32, (rows, rows), 0)
        gap = lax.broadcasted_iota(jnp.int32, (rows, rows), 1) - at_row
        laid = jnp.int32(0)
        total = None
        for k in range(strides):
            source = (e + shards - k) % shards
            count, start = segment(grids_ref, routing_ref, source, k)
            chosen = (at_row >= laid) & (at_row < laid + count) & (gap == start - laid)
            term = jnp.dot(chosen.astype(F32).astype(BF16), proj[source], preferred_element_type=F32)
            total = term if total is None else total + term
            laid = laid + count
        total = total.astype(BF16)
        for g in range(groups):
            if by_columns:
                part[e, g] = total[:, g * piece_cols:(g + 1) * piece_cols]
            else:
                part[e, g] = total[g * piece_rows:(g + 1) * piece_rows]
        for slot in (1, 0):
            swap_copy(e, slot).start()

    def cross(e):
        swap_copy(e, 1).wait_recv()
        cross_out[e] = (part[e, across].astype(F32) + pair_in[e, 1].astype(F32)).astype(BF16)
        cross_copy(e).start()

    def finish(e):
        swap_copy(e, 0).wait_recv()
        cross_copy(e).wait_recv()
        total = (part[e, group].astype(F32) + pair_in[e, 0].astype(F32) + cross_in[e].astype(F32)).astype(BF16)

        stays = (e == me) & (target == group)

        @pl.when(jnp.logical_not(stays))
        def _():
            ready_buf[e] = total
            out_copy(e, me, group).start()

        @pl.when(stays)
        def _():
            at_rows, at_cols = place_of(me, group)
            out_ref[at_rows, at_cols] = total

    def row_sums(values):
        squares = values * values
        lanes = squares[:, :LANES]
        for f in range(1, feature // LANES):
            lanes = lanes + squares[:, f * LANES:(f + 1) * LANES]
        return jnp.sum(lanes.T, axis=0, keepdims=True)

    def text_sums():
        text_copy.wait()

        def block(i, carry):
            span = pl.ds(pl.multiple_of(i * LANES, LANES), LANES)
            sums_out[:, span] = row_sums(text_buf[span, :].astype(F32))
            return carry

        lax.fori_loop(0, seq // LANES, block, 0)

    def is_block(block, away, way):
        return (away >= 0) & (away < length) & ((away > 0) | (way == 1)) & (block >= 0) & (block < length)

    def slot_step(step, c):
        @pl.when(step == 0)
        def _():
            hidden_chunk(c)

        for way in (1, -1):
            block = place - way * step
            have = (step < length) & (block >= 0) & (block < length)

            @pl.when(have & (step > 0))
            def _(block=block, way=way):
                line_copy(block, c, way).wait_recv()

            @pl.when(have & (place + way >= 0) & (place + way < length))
            def _(block=block, way=way):
                line_copy(block, c, way).start()

            @pl.when(is_block(block, step, way) & jnp.logical_not(by_line(block, c)))
            def _(block=block):
                pair_copy(block, c, row).start()

        for way in (1, -1):
            away = place if way == 1 else length - 1 - place

            chunk = c + jnp.where(away == 1, 0, cut)

            @pl.when((away > 0) & (step == away + 1) & (chunk < chunks))
            def _(away=away, way=way, chunk=chunk):
                extra_copy(chunk, way).wait_recv()

                @pl.when((away < length - 1) & (chunk >= cut))
                def _():
                    extra_copy(chunk, way).start()

        @pl.when((step == 1) & (c == 0))
        def _():
            second_copy.wait()

        @pl.when((step == 1) & (c == 3))
        def _():
            text_sums()

        @pl.when((step > 0) & (c > 0) & (c < 3))
        def _():
            def now(e):
                @pl.when((ready_step(e) == step - 1) & ((e + row) % 2 == c - 1))
                def _():
                    cross(e)

            over_shards(now)

        @pl.when((step > 0) & (c < 2))
        def _():
            def now(e):
                @pl.when((ready_step(e) == step - 1) & ((e + row) % 2 == c))
                def _():
                    pick(e)

            over_shards(now)

        @pl.when((step == length) & (c == 3))
        def _():
            def now(e):
                @pl.when((ready_step(e) <= length - 2) & ((e + row) % 2 == 0))
                def _():
                    finish(e)

            over_shards(now)

        def unit(i, carry):
            way = 1 - 2 * (i % 2)
            own = i == 2
            block = jnp.where(own, place, place - way * step)

            @pl.when((step > 0) & jnp.where(own, step == 1, (step < length) & (block >= 0) & (block < length)))
            def _():
                accumulate(2 * block + row, c, jnp.where(own, 4, (way + 1) // 2))

            return carry

        lax.fori_loop(0, 3, unit, 0)

        def other_unit(i, carry):
            way = 1 - 2 * (i % 2)
            block = place - way * (step - 1)
            far = i // 2
            plain = is_block(block, step - 1, way)
            split = ((block == 0) & (place != 0)) | ((block == length - 1) & (place != length - 1))
            near = (far == 0) & plain & jnp.logical_not(by_line(block, c))
            chunk = c + far * jnp.where(step == 2, 0, cut)

            @pl.when(near)
            def _():
                pair_copy(block, c, 1 - row).wait_recv()

            @pl.when(near | ((far == 1) & plain & split & (chunk < chunks)))
            def _():
                accumulate(2 * block + 1 - row, chunk, 2 + (way + 1) // 2)

            return carry

        lax.fori_loop(0, 4, other_unit, 0)

        for way, end in ((1, 0), (-1, length - 1)):

            @pl.when((step == 1) & (place == end))
            def _(way=way):
                extra_copy(c, way).start()

        @pl.when(c == chunks - 1)
        def _():
            def settle_unit(i, carry):
                way, kind = 1 - 2 * (i % 2), i // 2
                block = place - way * (step - kind)

                @pl.when(is_block(block, step - kind, way) & (step > 0))
                def _():
                    source = 2 * block + jnp.abs(row - kind)
                    proj[source] = sums[2 * kind + (way + 1) // 2].astype(BF16)

                return carry

            lax.fori_loop(0, 4, settle_unit, 0)

            @pl.when(step == 1)
            def _():
                proj[me] = sums[4].astype(BF16)

    def outer(step, carry):
        def inner(c, carry):
            slot_step(step, c)
            return carry

        return lax.fori_loop(0, chunks, inner, carry)

    steps = length + 1 + ((place == 0) | (place == length - 1)).astype(jnp.int32)
    lax.fori_loop(0, steps, outer, 0)

    def last_sends(i, carry):
        e, turn = (me + 1 + i) % shards, i // shards
        far, crosses = (e + row) % 2, ready_step(e)
        when = jnp.where(crosses == length, 3, jnp.where(crosses == length - 1, 0, 1 - 2 * (1 - far))) + jnp.where(crosses == length - 1, 2 * far, far * (crosses == length).astype(jnp.int32))

        @pl.when(when == turn)
        def _():
            finish(e)

        return carry

    lax.fori_loop(0, 5 * shards, last_sends, 0)

    filled = jnp.int32(0)
    for k in range(strides):
        filled = filled + segment(grids_ref, routing_ref, (me + shards - k) % shards, k)[0]
    if rows < top_rows:
        out_ref[rows:, :] = text_buf[rows:top_rows, :]
    lane_sums[...] = jnp.zeros_like(lane_sums)

    def splice(i, carry):
        sender, source = i % groups, group * per_group + i // groups

        @pl.when((sender != group) | (source != me))
        def _():
            out_copy(me, source, sender).wait_recv()

        at_rows, at_cols = place_of(source, sender)
        line = lax.broadcasted_iota(jnp.int32, (piece_rows, piece_cols), 0) + (0 if by_columns else sender * piece_rows)
        image = (out_ref[at_rows, at_cols].astype(F32) + second_bias_ref[at_cols][None, :]).astype(BF16)
        values = image.astype(F32)
        out_ref[at_rows, at_cols] = jnp.where(line < filled, values, text_buf[at_rows, at_cols].astype(F32)).astype(BF16)
        squares = values * values
        lanes = squares[:, :LANES]
        for f in range(1, piece_cols // LANES):
            lanes = lanes + squares[:, f * LANES:(f + 1) * LANES]
        lane_sums[at_rows, :] = lane_sums[at_rows, :] + lanes
        return carry

    lax.fori_loop(0, shards, splice, 0)
    for i in range(top_rows // LANES):
        span = slice(i * LANES, (i + 1) * LANES)
        line = lax.broadcasted_iota(jnp.int32, (1, LANES), 1) + i * LANES
        image = jnp.sum(lane_sums[span, :].T, axis=0, keepdims=True)
        sums_out[:, span] = jnp.where(line < filled, image, sums_out[:, span])
    top_copy = pltpu.make_async_copy(out_ref, top_ref, top_sem)

    def sums_copy(peer, sender, i):
        return pltpu.make_async_remote_copy(
            src_ref=sums_out,
            dst_ref=sums_in.at[sender],
            send_sem=sums_send.at[i],
            recv_sem=sums_recv.at[sender],
            device_id={"tensor": peer},
        )

    for i, peer in enumerate(peers):
        sums_copy(peer, group, i).start()
    top_copy.start()

    def drain_line(t, carry):
        block, c = t // chunks, t % chunks

        @pl.when(jnp.logical_not(by_line(block, c)))
        def _():
            pair_copy(block, c, row).wait_send()

        @pl.when((block <= place) & (place < length - 1))
        def _():
            line_copy(block, c, 1).wait_send()

        @pl.when((block >= place) & (place > 0))
        def _():
            line_copy(block, c, -1).wait_send()

        return carry

    lax.fori_loop(0, length * chunks, drain_line, 0)

    def drain_extra(c, carry):
        for way, start, end in ((1, 0, length - 1), (-1, length - 1, 0)):

            @pl.when((place != end) & ((c >= cut) | (place == start)))
            def _(way=way):
                extra_copy(c, way).wait_send()

        return carry

    lax.fori_loop(0, chunks, drain_extra, 0)

    def drain(e):
        for slot in (1, 0):
            swap_copy(e, slot).wait_send()
        cross_copy(e).wait_send()

        @pl.when((e != me) | (target != group))
        def _():
            out_copy(e, me, group).wait_send()

    over_shards(drain)
    total = sums_out[...]
    for i, peer in enumerate(peers):
        copy = sums_copy(peer, peer, i)
        copy.wait_recv()
        copy.wait_send()
        total = total + sums_in[peer]
    sums_ref[...] = total
    top_copy.wait()


def merge(rows, call_id, shards, groups, grids, routing, patches, norm_gain, norm_bias, first_weight, first_bias, second_weight, second_bias, text_embeds):
    patch_rows, vit = patches.shape
    per_token = first_weight.shape[0] // vit
    tokens = patch_rows // per_token
    hidden_width = first_weight.shape[1]
    chunks = hidden_width // CHUNK
    depth, width = second_weight.shape
    seq, feature = text_embeds.shape
    length = shards // 2
    by_columns = width % (groups * LANES) == 0
    piece = (rows, width // groups) if by_columns else (rows // groups, width)
    per_group = shards // groups
    dma = pltpu.SemaphoreType.DMA
    vmem = pl.BlockSpec(memory_space=pltpu.VMEM)
    anywhere = pl.BlockSpec(memory_space=pl.ANY)
    block = pltpu.VMEM((shards,) + piece, BF16)
    return pl.pallas_call(
        functools.partial(merge_kernel, rows, by_columns),
        in_specs=[anywhere, anywhere, anywhere, vmem, vmem, anywhere, vmem, anywhere, vmem, anywhere],
        out_specs=[anywhere, vmem],
        out_shape=[
            jax.ShapeDtypeStruct((tokens, feature), BF16),
            jax.ShapeDtypeStruct((1, seq), F32),
        ],
        scratch_shapes=[
            pltpu.SMEM(grids.shape, jnp.int32),
            pltpu.SMEM(routing.shape, jnp.int32),
            pltpu.VMEM((tokens, LANES), F32),
            pltpu.VMEM((tokens, feature), BF16),
            pltpu.VMEM((patch_rows, vit), BF16),
            pltpu.VMEM((LANES, vit), BF16),
            pltpu.VMEM((LANES, vit), BF16),
            pltpu.VMEM((per_token, tokens, vit), BF16),
            pltpu.VMEM((chunks, first_weight.shape[0], CHUNK), BF16),
            pltpu.VMEM((depth, width), BF16),
            pltpu.VMEM((seq, feature), BF16),
            pltpu.VMEM((rows, tokens), BF16),
            pltpu.VMEM((tokens, CHUNK), F32),
            pltpu.VMEM((shards, chunks, rows, CHUNK), BF16),
            pltpu.VMEM((5, rows, width), F32),
            pltpu.VMEM((shards, rows, width), BF16),
            pltpu.VMEM((shards, groups) + piece, BF16),
            pltpu.VMEM((shards, 2) + piece, BF16),
            block, block, block,
            pltpu.VMEM((1, seq), F32),
            pltpu.VMEM((groups, 1, seq), F32),
            dma, dma((2,)), dma((patch_rows // LANES,)), dma((chunks,)), dma, dma,
            dma((2, length, chunks)), dma((length, chunks)), dma((2, chunks)), dma((2, chunks)),
            dma((length, chunks)), dma((length, chunks)),
            dma((2, shards)), dma((2, shards)), dma((shards,)), dma((shards,)),
            dma((shards,)), dma((groups, per_group)),
            dma((groups - 1,)), dma((groups,)),
        ],
        compiler_params=pltpu.CompilerParams(
            collective_id=call_id, has_side_effects=True, vmem_limit_bytes=VMEM_LIMIT
        ),
        name="merge_%d" % rows,
    )(grids, routing, patches, norm_gain, norm_bias, first_weight, first_bias, second_weight, second_bias, text_embeds)


def scale_kernel(total_width, top_ref, text_ref, sums_ref, gain_ref, out_ref, normed_ref, rows_buf, normed_buf, in_sem, out_sem, normed_sem):
    feature = gain_ref.shape[0]
    blocks, top_blocks = rows_buf.shape[0], top_ref.shape[0] // LANES

    def in_copy(i):
        source = top_ref if i < top_blocks else text_ref
        return pltpu.make_async_copy(source.at[pl.ds(i * LANES, LANES)], rows_buf.at[i], in_sem.at[i])

    def span_of(i):
        return pl.ds(pl.multiple_of(i * LANES, LANES), LANES)

    def out_copy(i):
        return pltpu.make_async_copy(rows_buf.at[i], out_ref.at[span_of(i)], out_sem.at[i])

    def normed_copy(i):
        return pltpu.make_async_copy(normed_buf.at[i], normed_ref.at[span_of(i)], normed_sem.at[i])

    for i in range(blocks):
        in_copy(i).start()
    gain = gain_ref[...][None, :]

    for i in range(blocks):
        in_copy(i).wait()
        out_copy(i).start()
        scale = lax.rsqrt(sums_ref[:, pl.ds(i * LANES, LANES)] / total_width + 1e-06)
        scale = jnp.broadcast_to(scale, (LANES, LANES)).T
        for f in range(feature // LANES):
            span = slice(f * LANES, (f + 1) * LANES)
            normed_buf[i, :, span] = (rows_buf[i, :, span].astype(F32) * scale * gain[:, span]).astype(BF16)
        normed_copy(i).start()

    for i in range(blocks):
        out_copy(i).wait()
        normed_copy(i).wait()


def scale_rows(top, text_embeds, sums, final_gain, groups):
    seq, feature = text_embeds.shape
    anywhere = pl.BlockSpec(memory_space=pl.ANY)
    vmem = pl.BlockSpec(memory_space=pltpu.VMEM)
    blocks = seq // LANES
    dma = pltpu.SemaphoreType.DMA
    return pl.pallas_call(
        functools.partial(scale_kernel, feature * groups),
        in_specs=[anywhere, anywhere, vmem, vmem],
        out_specs=[anywhere, anywhere],
        out_shape=[jax.ShapeDtypeStruct((seq, feature), BF16)] * 2,
        scratch_shapes=[
            pltpu.VMEM((blocks, LANES, feature), BF16),
            pltpu.VMEM((blocks, LANES, feature), BF16),
            dma((blocks,)), dma((blocks,)), dma((blocks,)),
        ],
        compiler_params=pltpu.CompilerParams(vmem_limit_bytes=VMEM_LIMIT),
        name="scale_rows",
    )(top, text_embeds, sums, final_gain)


def bucket_sizes(slots, width, groups):
    step = slots // 16 if width % (groups * LANES) == 0 else slots // 4
    return tuple(b for b in range(slots // 2 + step, slots + 1, step) if b <= slots * 13 // 16 or b == slots)


def per_device(
    patches,
    norm_gain,
    norm_bias,
    first_weight,
    first_bias,
    second_weight,
    second_bias,
    text_embeds,
    final_gain,
    image_grids,
    routing,
):
    shards = lax.axis_size("dp")
    groups = lax.axis_size("tensor")
    slots = patches.shape[0] * patches.shape[1] // first_weight.shape[0]
    grids, offsets = image_grids.transpose(1, 2, 0), routing.T
    buckets = BUCKETS(slots, second_weight.shape[1], groups)
    which = pl.pallas_call(
        functools.partial(plan_kernel, buckets),
        in_specs=[pl.BlockSpec(memory_space=pl.ANY)] * 2,
        out_specs=pl.BlockSpec(memory_space=pltpu.SMEM),
        out_shape=jax.ShapeDtypeStruct((1,), jnp.int32),
        scratch_shapes=[
            pltpu.SMEM(grids.shape, jnp.int32),
            pltpu.SMEM(offsets.shape, jnp.int32),
            pltpu.SMEM((shards,), jnp.int32),
            pltpu.SemaphoreType.DMA((2,)),
        ],
        name="plan",
    )(grids, offsets)

    def branch(rows, call_id):
        return lambda: merge(
            rows, call_id, shards, groups, grids, offsets, patches, norm_gain, norm_bias,
            first_weight, first_bias, second_weight, second_bias, text_embeds,
        )

    top, sums = lax.switch(which[0], [branch(rows, i) for i, rows in enumerate(buckets)])
    return tuple(scale_rows(top, text_embeds, sums, final_gain, groups))


BUCKETS = bucket_sizes


def solution(mesh):
    placed = (
        P("dp", None),
        P(),
        P(),
        P(None, "tensor"),
        P("tensor"),
        P("tensor", "dp"),
        P("tensor"),
        P("dp", "tensor"),
        P("tensor"),
        P(),
        P(),
    )
    return jax.shard_map(
        per_device,
        mesh=mesh,
        in_specs=placed,
        out_specs=(P("dp", "tensor"), P("dp", "tensor")),
        check_vma=False,
    )
```

```python
import functools

import jax
import jax.numpy as jnp
from jax import lax
from jax.experimental import pallas as pl
from jax.experimental.pallas import tpu as pltpu
from jax.sharding import PartitionSpec as P

VMEM_LIMIT = 60 * 1024 * 1024
LANES = 128
CHUNK = 256
F32 = jnp.float32
BF16 = jnp.bfloat16


def area_of(grids_ref, s, b):
    return grids_ref[b, 0, s] * grids_ref[b, 1, s]


def segment(grids_ref, routing_ref, s, k):
    count, start = jnp.int32(0), jnp.int32(0)
    for b in range(routing_ref.shape[0]):
        area, offset = area_of(grids_ref, s, b), routing_ref[b, s]
        count = count + jnp.where(offset == k, area, 0)
        start = start + jnp.where(offset < k, area, 0)
    return count, start


def table_copies(grids_hbm, routing_hbm, grids_ref, routing_ref, table_sem):
    return (
        pltpu.make_async_copy(grids_hbm, grids_ref, table_sem.at[0]),
        pltpu.make_async_copy(routing_hbm, routing_ref, table_sem.at[1]),
    )


def plan_kernel(buckets, grids_hbm, routing_hbm, which_ref, grids_ref, routing_ref, filled_ref, table_sem):
    strides, shards = routing_ref.shape
    copies = table_copies(grids_hbm, routing_hbm, grids_ref, routing_ref, table_sem)
    for copy in copies:
        copy.start()
    for copy in copies:
        copy.wait()

    for e in range(shards):
        filled_ref[e] = 0
    most = jnp.int32(0)
    for s in range(shards):
        sent = jnp.int32(0)
        for b in range(strides):
            area = area_of(grids_ref, s, b)
            sent = sent + area
            e = s + routing_ref[b, s]
            e = jnp.where(e >= shards, e - shards, e)
            filled_ref[e] = filled_ref[e] + area
        most = jnp.maximum(most, sent)
    for e in range(shards):
        most = jnp.maximum(most, filled_ref[e])
    which = jnp.int32(0)
    for bucket in buckets[:-1]:
        which = which + (most > bucket).astype(jnp.int32)
    which_ref[0] = which


def merge_kernel(
    rows, by_columns,
    grids_hbm, routing_hbm, patches_ref, gain_ref, bias_ref, first_ref, first_bias_ref, second_ref, second_bias_ref, text_ref,
    embed_ref, sums_ref,
    grids_ref, routing_ref, lane_sums, out_ref, patch_buf, norm_a, norm_b, merged, first_buf, second_buf, own_pick, acc, gath, sums, proj,
    part, pair_in, cross_out, cross_in, ready_buf, sums_out, sums_in,
    table_sem, patch_sem, first_sem, second_sem, text_sem,
    line_send, line_recv, extra_send, extra_recv, pair_send, pair_recv, swap_send, swap_recv, cross_send, cross_recv,
    out_send, out_recv, sums_send, sums_recv,
):
    shards, chunks = gath.shape[0], gath.shape[1]
    strides = routing_ref.shape[0]
    groups, piece_rows, piece_cols = part.shape[1:]
    per_group = shards // groups
    length = shards // 2
    per_token, tokens, vit = merged.shape
    cap = tokens // strides
    depth, width = second_buf.shape
    cut = (chunks + 1) // 2
    ln_rows = LANES
    ln_steps = patch_buf.shape[0] // ln_rows
    ln_tokens = ln_rows // per_token
    seq, feature = embed_ref.shape
    top_rows = out_ref.shape[0]

    me = lax.axis_index("dp")
    group = lax.axis_index("tensor")
    place, row = me // 2, me % 2
    other = me + 1 - 2 * row
    core, side = group % 2, group // 2
    mate = 2 * side + 1 - core
    across = group + 2 - 4 * side
    across_mate = mate + 2 - 4 * side
    peers = (mate, across, across_mate)

    target = me // per_group
    barrier = pltpu.get_barrier_semaphore()
    pl.semaphore_signal(barrier, inc=1, device_id={"dp": other})
    for way, end in ((1, length - 1), (-1, 0)):

        @pl.when(place != end)
        def _(way=way):
            pl.semaphore_signal(barrier, inc=1, device_id={"dp": me + 2 * way})

    for peer in peers:
        pl.semaphore_signal(barrier, inc=1, device_id={"tensor": peer})

    def over_senders(body):
        def run(i, carry):
            sender, source = i % groups, group * per_group + i // groups

            @pl.when((sender != group) | (source != me))
            def _():
                body(source, sender)

            return carry

        lax.fori_loop(0, shards, run, 0)

    def greet(source, sender):
        pl.semaphore_signal(barrier, inc=1, device_id={"dp": source, "tensor": sender})

    over_senders(greet)
    near = 1 + (place > 0).astype(jnp.int32) + (place < length - 1).astype(jnp.int32)
    greeted = near + len(peers) + shards - (target == group).astype(jnp.int32)

    def patch_copy(i):
        span = pl.ds(pl.multiple_of(i * ln_rows, ln_rows), ln_rows)
        return pltpu.make_async_copy(patches_ref.at[span, :], patch_buf.at[span, :], patch_sem.at[i])

    def first_copy(c):
        span = pl.ds(pl.multiple_of(c * CHUNK, CHUNK), CHUNK)
        return pltpu.make_async_copy(first_ref.at[:, span], first_buf.at[c], first_sem.at[c])

    second_copy = pltpu.make_async_copy(second_ref, second_buf, second_sem)
    text_copy = pltpu.make_async_copy(text_ref, embed_ref, text_sem)

    def start_patch(i, carry):
        patch_copy(i).start()
        return carry

    lax.fori_loop(0, ln_steps, start_patch, 0)
    tables = table_copies(grids_hbm, routing_hbm, grids_ref, routing_ref, table_sem)
    for table in tables:
        table.start()

    gain = gain_ref[...][None, :]
    bias = bias_ref[...][None, :]
    def norm_rows(i, norm_buf):
        patch_copy(i).wait()
        values = patch_buf[pl.ds(pl.multiple_of(i * ln_rows, ln_rows), ln_rows), :].astype(F32)
        centered = values - jnp.mean(values, axis=-1, keepdims=True)
        variance = jnp.mean(centered * centered, axis=-1, keepdims=True)
        normed = centered * lax.rsqrt(variance + 1e-06) * gain + bias
        for f in range(vit // LANES):
            norm_buf[f] = normed[:, f * LANES:(f + 1) * LANES]

    def merge_rows(i, norm_buf):
        for j in range(per_token):
            strips = [norm_buf[f, pl.ds(j, ln_tokens, stride=per_token), :] for f in range(vit // LANES)]
            merged[j, pl.ds(pl.multiple_of(i * ln_tokens, ln_tokens), ln_tokens), :] = jnp.concatenate(strips, axis=1).astype(BF16)

    def norm_pair(h, carry):
        for i in (2 * h, 2 * h + 1):

            @pl.when(i < chunks)
            def _(i=i):
                first_copy(i).start()

        @pl.when(h == ln_steps // 2 - 1)
        def _():
            second_copy.start()
            text_copy.start()

        norm_rows(2 * h, norm_a)
        norm_rows(2 * h + 1, norm_b)
        merge_rows(2 * h, norm_a)
        merge_rows(2 * h + 1, norm_b)
        return carry

    lax.fori_loop(0, ln_steps // 2, norm_pair, 0)
    for table in tables:
        table.wait()

    token_row = lax.broadcasted_iota(jnp.int32, (rows, tokens), 0)
    token_gap = lax.broadcasted_iota(jnp.int32, (rows, tokens), 1) - token_row
    picked = jnp.zeros((rows, tokens), jnp.bool_)
    for b in range(strides):
        offset = routing_ref[b, me]
        start = jnp.int32(0)
        for o in range(strides):
            start = start + jnp.where(routing_ref[o, me] < offset, area_of(grids_ref, me, o), 0)
        stop = start + area_of(grids_ref, me, b)
        picked = picked | ((token_row >= start) & (token_row < stop) & (token_gap == b * cap - start))
    own_pick[...] = picked.astype(F32).astype(BF16)

    pl.semaphore_wait(barrier, greeted)

    def hidden_chunk(c):
        first_copy(c).wait()

        def add(j, carry):
            weight = first_buf[c, pl.ds(pl.multiple_of(j * vit, vit), vit), :]
            term = jnp.dot(merged[j], weight, preferred_element_type=F32)
            acc[...] = jnp.where(j == 0, term, acc[...] + term)
            return carry

        lax.fori_loop(0, per_token, add, 0)
        x = acc[...] + first_bias_ref[pl.ds(pl.multiple_of(c * CHUNK, CHUNK), CHUNK)][None, :]
        hidden = (0.5 * x * (1.0 + lax.erf(x * (0.5 ** 0.5)))).astype(BF16)
        gath[me, c] = jnp.dot(own_pick[...], hidden, preferred_element_type=F32).astype(BF16)

    def line_copy(block, c, way):
        here = gath.at[2 * block + row, c]
        return pltpu.make_async_remote_copy(
            src_ref=here,
            dst_ref=here,
            send_sem=line_send.at[(way + 1) // 2, block, c],
            recv_sem=line_recv.at[block, c],
            device_id={"dp": me + 2 * way},
        )

    def by_line(block, c):
        first = (block == 0) & (place != 0) & ((c >= cut) | (place == 1))
        last = (block == length - 1) & (place != length - 1) & ((c >= cut) | (place == length - 2))
        return first | last

    def extra_copy(c, way):
        here = gath.at[(length - 1) * (1 - way) + 1 - row, c]
        return pltpu.make_async_remote_copy(
            src_ref=here,
            dst_ref=here,
            send_sem=extra_send.at[(way + 1) // 2, c],
            recv_sem=extra_recv.at[(way + 1) // 2, c],
            device_id={"dp": me + 2 * way},
        )

    def pair_copy(block, c, side_row):
        here = gath.at[2 * block + side_row, c]
        return pltpu.make_async_remote_copy(
            src_ref=here,
            dst_ref=here,
            send_sem=pair_send.at[block, c],
            recv_sem=pair_recv.at[block, c],
            device_id={"dp": other},
        )

    def swap_copy(e, slot):
        return pltpu.make_async_remote_copy(
            src_ref=part.at[e, mate if slot == 0 else across_mate],
            dst_ref=pair_in.at[e, slot],
            send_sem=swap_send.at[slot, e],
            recv_sem=swap_recv.at[slot, e],
            device_id={"tensor": mate},
        )

    def cross_copy(e):
        return pltpu.make_async_remote_copy(
            src_ref=cross_out.at[e],
            dst_ref=cross_in.at[e],
            send_sem=cross_send.at[e],
            recv_sem=cross_recv.at[e],
            device_id={"tensor": across},
        )

    def place_of(source, sender):
        if by_columns:
            at = ((source % per_group) * groups + sender) * piece_cols
            return pl.ds(0, rows), pl.ds(pl.multiple_of(at, piece_cols), piece_cols)
        return (
            pl.ds(pl.multiple_of(sender * piece_rows, piece_rows), piece_rows),
            pl.ds(pl.multiple_of((source % per_group) * piece_cols, piece_cols), piece_cols),
        )

    def out_copy(e, source, sender):
        return pltpu.make_async_remote_copy(
            src_ref=ready_buf.at[e],
            dst_ref=out_ref.at[place_of(source, sender)],
            send_sem=out_send.at[e],
            recv_sem=out_recv.at[sender, source % per_group],
            device_id={"dp": e, "tensor": target},
        )

    def compute_ready(e):
        last = jnp.int32(0)
        for k in range(strides):
            source = (e + shards - k) % shards
            away = jnp.abs(source // 2 - place) + jnp.abs(source % 2 - row)
            last = jnp.maximum(last, away)
        return last

    packed = jnp.int32(0)
    if shards <= 8:
        for e in range(shards):
            packed = packed + compute_ready(jnp.int32(e)) * (1 << (3 * e))

    def ready_step(e):
        return (packed >> (3 * e)) & 7 if shards <= 8 else compute_ready(e)

    def over_shards(body):
        def run(i, carry):
            body((me + 1 + i) % shards)
            return carry

        lax.fori_loop(0, shards, run, 0)

    def accumulate(source, c, slot):
        weight = second_buf[pl.ds(pl.multiple_of(c * CHUNK, CHUNK), CHUNK), :]
        term = jnp.dot(gath[source, c], weight, preferred_element_type=F32)
        sums[slot] = jnp.where(c == 0, term, sums[slot] + term)

    def pick(e):
        at_row = lax.broadcasted_iota(jnp.int32, (rows, rows), 0)
        gap = lax.broadcasted_iota(jnp.int32, (rows, rows), 1) - at_row
        laid = jnp.int32(0)
        total = None
        for k in range(strides):
            source = (e + shards - k) % shards
            count, start = segment(grids_ref, routing_ref, source, k)
            chosen = (at_row >= laid) & (at_row < laid + count) & (gap == start - laid)
            term = jnp.dot(chosen.astype(F32).astype(BF16), proj[source], preferred_element_type=F32)
            total = term if total is None else total + term
            laid = laid + count
        total = total.astype(BF16)
        for g in range(groups):
            if by_columns:
                part[e, g] = total[:, g * piece_cols:(g + 1) * piece_cols]
            else:
                part[e, g] = total[g * piece_rows:(g + 1) * piece_rows]
        for slot in (1, 0):
            swap_copy(e, slot).start()

    def cross(e):
        swap_copy(e, 1).wait_recv()
        cross_out[e] = (part[e, across].astype(F32) + pair_in[e, 1].astype(F32)).astype(BF16)
        cross_copy(e).start()

    def finish(e):
        swap_copy(e, 0).wait_recv()
        cross_copy(e).wait_recv()
        total = (part[e, group].astype(F32) + pair_in[e, 0].astype(F32) + cross_in[e].astype(F32)).astype(BF16)

        stays = (e == me) & (target == group)

        @pl.when(jnp.logical_not(stays))
        def _():
            ready_buf[e] = total
            out_copy(e, me, group).start()

        @pl.when(stays)
        def _():
            at_rows, at_cols = place_of(me, group)
            out_ref[at_rows, at_cols] = total

    def row_sums(values):
        squares = values * values
        lanes = squares[:, :LANES]
        for f in range(1, feature // LANES):
            lanes = lanes + squares[:, f * LANES:(f + 1) * LANES]
        return jnp.sum(lanes.T, axis=0, keepdims=True)

    def text_sums():
        text_copy.wait()

        def block(i, carry):
            span = pl.ds(pl.multiple_of(i * LANES, LANES), LANES)
            sums_out[:, span] = row_sums(embed_ref[span, :].astype(F32))
            return carry

        lax.fori_loop(0, seq // LANES, block, 0)

    def is_block(block, away, way):
        return (away >= 0) & (away < length) & ((away > 0) | (way == 1)) & (block >= 0) & (block < length)

    def slot_step(step, c):
        @pl.when(step == 0)
        def _():
            hidden_chunk(c)

        for way in (1, -1):
            block = place - way * step
            have = (step < length) & (block >= 0) & (block < length)

            @pl.when(have & (step > 0))
            def _(block=block, way=way):
                line_copy(block, c, way).wait_recv()

            @pl.when(have & (place + way >= 0) & (place + way < length))
            def _(block=block, way=way):
                line_copy(block, c, way).start()

            @pl.when(is_block(block, step, way) & jnp.logical_not(by_line(block, c)))
            def _(block=block):
                pair_copy(block, c, row).start()

        for way in (1, -1):
            away = place if way == 1 else length - 1 - place

            chunk = c + jnp.where(away == 1, 0, cut)

            @pl.when((away > 0) & (step == away + 1) & (chunk < chunks))
            def _(away=away, way=way, chunk=chunk):
                extra_copy(chunk, way).wait_recv()

                @pl.when((away < length - 1) & (chunk >= cut))
                def _():
                    extra_copy(chunk, way).start()

        @pl.when((step == 1) & (c == 0))
        def _():
            second_copy.wait()

        @pl.when((step == 1) & (c == 3))
        def _():
            text_sums()

        @pl.when((step > 0) & (c > 0) & (c < 3))
        def _():
            def now(e):
                @pl.when((ready_step(e) == step - 1) & ((e + row) % 2 == c - 1))
                def _():
                    cross(e)

            over_shards(now)

        @pl.when((step > 0) & (c < 2))
        def _():
            def now(e):
                @pl.when((ready_step(e) == step - 1) & ((e + row) % 2 == c))
                def _():
                    pick(e)

            over_shards(now)

        @pl.when((step == length) & (c == 3))
        def _():
            def now(e):
                @pl.when((ready_step(e) <= length - 2) & ((e + row) % 2 == 0))
                def _():
                    finish(e)

            over_shards(now)

        def unit(i, carry):
            way = 1 - 2 * (i % 2)
            own = i == 2
            block = jnp.where(own, place, place - way * step)

            @pl.when((step > 0) & jnp.where(own, step == 1, (step < length) & (block >= 0) & (block < length)))
            def _():
                accumulate(2 * block + row, c, jnp.where(own, 4, (way + 1) // 2))

            return carry

        lax.fori_loop(0, 3, unit, 0)

        def other_unit(i, carry):
            way = 1 - 2 * (i % 2)
            block = place - way * (step - 1)
            far = i // 2
            plain = is_block(block, step - 1, way)
            split = ((block == 0) & (place != 0)) | ((block == length - 1) & (place != length - 1))
            near = (far == 0) & plain & jnp.logical_not(by_line(block, c))
            chunk = c + far * jnp.where(step == 2, 0, cut)

            @pl.when(near)
            def _():
                pair_copy(block, c, 1 - row).wait_recv()

            @pl.when(near | ((far == 1) & plain & split & (chunk < chunks)))
            def _():
                accumulate(2 * block + 1 - row, chunk, 2 + (way + 1) // 2)

            return carry

        lax.fori_loop(0, 4, other_unit, 0)

        for way, end in ((1, 0), (-1, length - 1)):

            @pl.when((step == 1) & (place == end))
            def _(way=way):
                extra_copy(c, way).start()

        @pl.when(c == chunks - 1)
        def _():
            def settle_unit(i, carry):
                way, kind = 1 - 2 * (i % 2), i // 2
                block = place - way * (step - kind)

                @pl.when(is_block(block, step - kind, way) & (step > 0))
                def _():
                    source = 2 * block + jnp.abs(row - kind)
                    proj[source] = sums[2 * kind + (way + 1) // 2].astype(BF16)

                return carry

            lax.fori_loop(0, 4, settle_unit, 0)

            @pl.when(step == 1)
            def _():
                proj[me] = sums[4].astype(BF16)

    def outer(step, carry):
        def inner(c, carry):
            slot_step(step, c)
            return carry

        return lax.fori_loop(0, chunks, inner, carry)

    steps = length + 1 + ((place == 0) | (place == length - 1)).astype(jnp.int32)
    lax.fori_loop(0, steps, outer, 0)

    def last_sends(i, carry):
        e, turn = (me + 1 + i) % shards, i // shards
        far, crosses = (e + row) % 2, ready_step(e)
        when = jnp.where(crosses == length, 3, jnp.where(crosses == length - 1, 0, 1 - 2 * (1 - far))) + jnp.where(crosses == length - 1, 2 * far, far * (crosses == length).astype(jnp.int32))

        @pl.when(when == turn)
        def _():
            finish(e)

        return carry

    lax.fori_loop(0, 5 * shards, last_sends, 0)

    filled = jnp.int32(0)
    for k in range(strides):
        filled = filled + segment(grids_ref, routing_ref, (me + shards - k) % shards, k)[0]
    lane_sums[...] = jnp.zeros_like(lane_sums)

    def splice(i, carry):
        sender, source = i % groups, group * per_group + i // groups

        @pl.when((sender != group) | (source != me))
        def _():
            out_copy(me, source, sender).wait_recv()

        at_rows, at_cols = place_of(source, sender)
        line = lax.broadcasted_iota(jnp.int32, (piece_rows, piece_cols), 0) + (0 if by_columns else sender * piece_rows)
        image = (out_ref[at_rows, at_cols].astype(F32) + second_bias_ref[at_cols][None, :]).astype(BF16)
        values = image.astype(F32)
        embed_ref[at_rows, at_cols] = jnp.where(line < filled, values, embed_ref[at_rows, at_cols].astype(F32)).astype(BF16)
        squares = values * values
        lanes = squares[:, :LANES]
        for f in range(1, piece_cols // LANES):
            lanes = lanes + squares[:, f * LANES:(f + 1) * LANES]
        lane_sums[at_rows, :] = lane_sums[at_rows, :] + lanes
        return carry

    lax.fori_loop(0, shards, splice, 0)
    for i in range(top_rows // LANES):
        span = slice(i * LANES, (i + 1) * LANES)
        line = lax.broadcasted_iota(jnp.int32, (1, LANES), 1) + i * LANES
        image = jnp.sum(lane_sums[span, :].T, axis=0, keepdims=True)
        sums_out[:, span] = jnp.where(line < filled, image, sums_out[:, span])

    def sums_copy(peer, sender, i):
        return pltpu.make_async_remote_copy(
            src_ref=sums_out,
            dst_ref=sums_in.at[sender],
            send_sem=sums_send.at[i],
            recv_sem=sums_recv.at[sender],
            device_id={"tensor": peer},
        )

    for i, peer in enumerate(peers):
        sums_copy(peer, group, i).start()

    def drain_line(t, carry):
        block, c = t // chunks, t % chunks

        @pl.when(jnp.logical_not(by_line(block, c)))
        def _():
            pair_copy(block, c, row).wait_send()

        @pl.when((block <= place) & (place < length - 1))
        def _():
            line_copy(block, c, 1).wait_send()

        @pl.when((block >= place) & (place > 0))
        def _():
            line_copy(block, c, -1).wait_send()

        return carry

    lax.fori_loop(0, length * chunks, drain_line, 0)

    def drain_extra(c, carry):
        for way, start, end in ((1, 0, length - 1), (-1, length - 1, 0)):

            @pl.when((place != end) & ((c >= cut) | (place == start)))
            def _(way=way):
                extra_copy(c, way).wait_send()

        return carry

    lax.fori_loop(0, chunks, drain_extra, 0)

    def drain(e):
        for slot in (1, 0):
            swap_copy(e, slot).wait_send()
        cross_copy(e).wait_send()

        @pl.when((e != me) | (target != group))
        def _():
            out_copy(e, me, group).wait_send()

    over_shards(drain)
    total = sums_out[...]
    for i, peer in enumerate(peers):
        copy = sums_copy(peer, peer, i)
        copy.wait_recv()
        copy.wait_send()
        total = total + sums_in[peer]
    sums_ref[...] = total


def merge(rows, call_id, shards, groups, grids, routing, patches, norm_gain, norm_bias, first_weight, first_bias, second_weight, second_bias, text_embeds):
    patch_rows, vit = patches.shape
    per_token = first_weight.shape[0] // vit
    tokens = patch_rows // per_token
    hidden_width = first_weight.shape[1]
    chunks = hidden_width // CHUNK
    depth, width = second_weight.shape
    seq, feature = text_embeds.shape
    length = shards // 2
    by_columns = width % (groups * LANES) == 0
    piece = (rows, width // groups) if by_columns else (rows // groups, width)
    per_group = shards // groups
    dma = pltpu.SemaphoreType.DMA
    vmem = pl.BlockSpec(memory_space=pltpu.VMEM)
    anywhere = pl.BlockSpec(memory_space=pl.ANY)
    block = pltpu.VMEM((shards,) + piece, BF16)
    return pl.pallas_call(
        functools.partial(merge_kernel, rows, by_columns),
        in_specs=[anywhere, anywhere, anywhere, vmem, vmem, anywhere, vmem, anywhere, vmem, anywhere],
        out_specs=[vmem, vmem],
        out_shape=[
            jax.ShapeDtypeStruct((seq, feature), BF16),
            jax.ShapeDtypeStruct((1, seq), F32),
        ],
        scratch_shapes=[
            pltpu.SMEM(grids.shape, jnp.int32),
            pltpu.SMEM(routing.shape, jnp.int32),
            pltpu.VMEM((tokens, LANES), F32),
            pltpu.VMEM((tokens, feature), BF16),
            pltpu.VMEM((patch_rows, vit), BF16),
            pltpu.VMEM((vit // LANES, LANES, LANES), F32),
            pltpu.VMEM((vit // LANES, LANES, LANES), F32),
            pltpu.VMEM((per_token, tokens, vit), BF16),
            pltpu.VMEM((chunks, first_weight.shape[0], CHUNK), BF16),
            pltpu.VMEM((depth, width), BF16),
            pltpu.VMEM((rows, tokens), BF16),
            pltpu.VMEM((tokens, CHUNK), F32),
            pltpu.VMEM((shards, chunks, rows, CHUNK), BF16),
            pltpu.VMEM((5, rows, width), F32),
            pltpu.VMEM((shards, rows, width), BF16),
            pltpu.VMEM((shards, groups) + piece, BF16),
            pltpu.VMEM((shards, 2) + piece, BF16),
            block, block, block,
            pltpu.VMEM((1, seq), F32),
            pltpu.VMEM((groups, 1, seq), F32),
            dma((2,)), dma((patch_rows // LANES,)), dma((chunks,)), dma, dma,
            dma((2, length, chunks)), dma((length, chunks)), dma((2, chunks)), dma((2, chunks)),
            dma((length, chunks)), dma((length, chunks)),
            dma((2, shards)), dma((2, shards)), dma((shards,)), dma((shards,)),
            dma((shards,)), dma((groups, per_group)),
            dma((groups - 1,)), dma((groups,)),
        ],
        compiler_params=pltpu.CompilerParams(
            collective_id=call_id, has_side_effects=True, vmem_limit_bytes=VMEM_LIMIT
        ),
        name="merge_%d" % rows,
    )(grids, routing, patches, norm_gain, norm_bias, first_weight, first_bias, second_weight, second_bias, text_embeds)


def scale_kernel(total_width, embed_ref, sums_ref, gain_ref, out_ref, normed_ref, normed_buf, out_sem, normed_sem):
    feature = gain_ref.shape[0]
    blocks = normed_buf.shape[0]
    out_copy = pltpu.make_async_copy(embed_ref, out_ref, out_sem)
    out_copy.start()

    def normed_copy(i):
        return pltpu.make_async_copy(normed_buf.at[i], normed_ref.at[pl.ds(i * LANES, LANES)], normed_sem.at[i])

    for i in range(blocks):
        span = slice(i * LANES, (i + 1) * LANES)
        scale = lax.rsqrt(sums_ref[:, span] / total_width + 1e-06)
        scale = jnp.broadcast_to(scale, (LANES, LANES)).T
        for f in range(feature // LANES):
            at = slice(f * LANES, (f + 1) * LANES)
            normed_buf[i, :, at] = (embed_ref[span, at].astype(F32) * scale * gain_ref[at][None, :]).astype(BF16)
        normed_copy(i).start()

    out_copy.wait()
    for i in range(blocks):
        normed_copy(i).wait()


def scale_rows(embeddings, sums, final_gain, groups):
    seq, feature = embeddings.shape
    anywhere = pl.BlockSpec(memory_space=pl.ANY)
    vmem = pl.BlockSpec(memory_space=pltpu.VMEM)
    blocks = seq // LANES
    dma = pltpu.SemaphoreType.DMA
    return pl.pallas_call(
        functools.partial(scale_kernel, feature * groups),
        in_specs=[vmem, vmem, vmem],
        out_specs=[anywhere, anywhere],
        out_shape=[jax.ShapeDtypeStruct((seq, feature), BF16)] * 2,
        scratch_shapes=[pltpu.VMEM((blocks, LANES, feature), BF16), dma, dma((blocks,))],
        compiler_params=pltpu.CompilerParams(vmem_limit_bytes=VMEM_LIMIT),
        name="scale_rows",
    )(embeddings, sums, final_gain)


def bucket_sizes(slots, width, groups):
    step = slots // 16 if width % (groups * LANES) == 0 else slots // 4
    return tuple(b for b in range(slots // 2 + step, slots + 1, step) if b <= slots * 13 // 16 or b == slots)


def per_device(
    patches,
    norm_gain,
    norm_bias,
    first_weight,
    first_bias,
    second_weight,
    second_bias,
    text_embeds,
    final_gain,
    image_grids,
    routing,
):
    shards = lax.axis_size("dp")
    groups = lax.axis_size("tensor")
    slots = patches.shape[0] * patches.shape[1] // first_weight.shape[0]
    grids, offsets = image_grids.transpose(1, 2, 0), routing.T
    buckets = BUCKETS(slots, second_weight.shape[1], groups)
    which = pl.pallas_call(
        functools.partial(plan_kernel, buckets),
        in_specs=[pl.BlockSpec(memory_space=pl.ANY)] * 2,
        out_specs=pl.BlockSpec(memory_space=pltpu.SMEM),
        out_shape=jax.ShapeDtypeStruct((1,), jnp.int32),
        scratch_shapes=[
            pltpu.SMEM(grids.shape, jnp.int32),
            pltpu.SMEM(offsets.shape, jnp.int32),
            pltpu.SMEM((shards,), jnp.int32),
            pltpu.SemaphoreType.DMA((2,)),
        ],
        name="plan",
    )(grids, offsets)

    def branch(rows, call_id):
        return lambda: merge(
            rows, call_id, shards, groups, grids, offsets, patches, norm_gain, norm_bias,
            first_weight, first_bias, second_weight, second_bias, text_embeds,
        )

    embeddings, sums = lax.switch(which[0], [branch(rows, i) for i, rows in enumerate(buckets)])
    return tuple(scale_rows(embeddings, sums, final_gain, groups))


BUCKETS = bucket_sizes


def solution(mesh):
    placed = (
        P("dp", None),
        P(),
        P(),
        P(None, "tensor"),
        P("tensor"),
        P("tensor", "dp"),
        P("tensor"),
        P("dp", "tensor"),
        P("tensor"),
        P(),
        P(),
    )
    return jax.shard_map(
        per_device,
        mesh=mesh,
        in_specs=placed,
        out_specs=(P("dp", "tensor"), P("dp", "tensor")),
        check_vma=False,
    )
```

```python
import functools

import jax
import jax.numpy as jnp
from jax import lax
from jax.experimental import pallas as pl
from jax.experimental.pallas import tpu as pltpu
from jax.sharding import PartitionSpec as P

VMEM_LIMIT = 60 * 1024 * 1024
LANES = 128
CHUNK = 256
F32 = jnp.float32
BF16 = jnp.bfloat16


def area_of(grids_ref, s, b):
    return grids_ref[b, 0, s] * grids_ref[b, 1, s]


def segment(grids_ref, routing_ref, s, k):
    count, start = jnp.int32(0), jnp.int32(0)
    for b in range(routing_ref.shape[0]):
        area, offset = area_of(grids_ref, s, b), routing_ref[b, s]
        count = count + jnp.where(offset == k, area, 0)
        start = start + jnp.where(offset < k, area, 0)
    return count, start


def table_copies(grids_hbm, routing_hbm, grids_ref, routing_ref, table_sem):
    return (
        pltpu.make_async_copy(grids_hbm, grids_ref, table_sem.at[0]),
        pltpu.make_async_copy(routing_hbm, routing_ref, table_sem.at[1]),
    )


def plan_kernel(buckets, grids_hbm, routing_hbm, which_ref, grids_ref, routing_ref, filled_ref, table_sem):
    strides, shards = routing_ref.shape
    copies = table_copies(grids_hbm, routing_hbm, grids_ref, routing_ref, table_sem)
    for copy in copies:
        copy.start()
    for copy in copies:
        copy.wait()

    for e in range(shards):
        filled_ref[e] = 0
    most = jnp.int32(0)
    for s in range(shards):
        sent = jnp.int32(0)
        for b in range(strides):
            area = area_of(grids_ref, s, b)
            sent = sent + area
            e = s + routing_ref[b, s]
            e = jnp.where(e >= shards, e - shards, e)
            filled_ref[e] = filled_ref[e] + area
        most = jnp.maximum(most, sent)
    for e in range(shards):
        most = jnp.maximum(most, filled_ref[e])
    which = jnp.int32(0)
    for bucket in buckets[:-1]:
        which = which + (most > bucket).astype(jnp.int32)
    which_ref[0] = which


def merge_kernel(
    rows, by_columns,
    grids_hbm, routing_hbm, patches_ref, gain_ref, bias_ref, first_ref, first_bias_ref, second_ref, second_bias_ref, text_ref,
    embed_ref, sums_ref,
    grids_ref, routing_ref, lane_sums, out_ref, patch_buf, norm_a, norm_b, merged, first_buf, second_buf, own_pick, acc, gath, sums, proj,
    part, pair_in, cross_out, cross_in, ready_buf, sums_out, sums_in,
    table_sem, patch_sem, first_sem, second_sem, text_sem,
    line_send, line_recv, extra_send, extra_recv, pair_send, pair_recv, swap_send, swap_recv, cross_send, cross_recv,
    out_send, out_recv, sums_send, sums_recv,
):
    shards, chunks = gath.shape[0], gath.shape[1]
    strides = routing_ref.shape[0]
    groups, piece_rows, piece_cols = part.shape[1:]
    per_group = shards // groups
    length = shards // 2
    per_token, tokens, vit = merged.shape
    cap = tokens // strides
    depth, width = second_buf.shape
    cut = (chunks + 1) // 2
    assert cut >= chunks - cut and chunks - cut >= 2
    ln_rows = LANES
    ln_steps = patch_buf.shape[0] // ln_rows
    ln_tokens = ln_rows // per_token
    seq, feature = embed_ref.shape
    top_rows = out_ref.shape[0]

    me = lax.axis_index("dp")
    group = lax.axis_index("tensor")
    place, row = me // 2, me % 2
    other = me + 1 - 2 * row
    core, side = group % 2, group // 2
    mate = 2 * side + 1 - core
    across = group + 2 - 4 * side
    across_mate = mate + 2 - 4 * side
    peers = (mate, across, across_mate)

    target = me // per_group
    barrier = pltpu.get_barrier_semaphore()
    pl.semaphore_signal(barrier, inc=1, device_id={"dp": other})
    for way, end in ((1, length - 1), (-1, 0)):

        @pl.when(place != end)
        def _(way=way):
            pl.semaphore_signal(barrier, inc=1, device_id={"dp": me + 2 * way})

    for peer in peers:
        pl.semaphore_signal(barrier, inc=1, device_id={"tensor": peer})

    def over_senders(body):
        def run(i, carry):
            sender, source = i % groups, group * per_group + i // groups

            @pl.when((sender != group) | (source != me))
            def _():
                body(source, sender)

            return carry

        lax.fori_loop(0, shards, run, 0)

    def greet(source, sender):
        pl.semaphore_signal(barrier, inc=1, device_id={"dp": source, "tensor": sender})

    over_senders(greet)
    near = 1 + (place > 0).astype(jnp.int32) + (place < length - 1).astype(jnp.int32)
    greeted = near + len(peers) + shards - (target == group).astype(jnp.int32)

    def patch_copy(i):
        span = pl.ds(pl.multiple_of(i * ln_rows, ln_rows), ln_rows)
        return pltpu.make_async_copy(patches_ref.at[span, :], patch_buf.at[span, :], patch_sem.at[i])

    def first_copy(c):
        span = pl.ds(pl.multiple_of(c * CHUNK, CHUNK), CHUNK)
        return pltpu.make_async_copy(first_ref.at[:, span], first_buf.at[c], first_sem.at[c])

    second_copy = pltpu.make_async_copy(second_ref, second_buf, second_sem)
    text_copy = pltpu.make_async_copy(text_ref, embed_ref, text_sem)

    def start_patch(i, carry):
        patch_copy(i).start()
        return carry

    lax.fori_loop(0, ln_steps, start_patch, 0)
    tables = table_copies(grids_hbm, routing_hbm, grids_ref, routing_ref, table_sem)
    for table in tables:
        table.start()

    gain = gain_ref[...][None, :]
    bias = bias_ref[...][None, :]
    def norm_rows(i, norm_buf):
        patch_copy(i).wait()
        values = patch_buf[pl.ds(pl.multiple_of(i * ln_rows, ln_rows), ln_rows), :].astype(F32)
        centered = values - jnp.mean(values, axis=-1, keepdims=True)
        variance = jnp.mean(centered * centered, axis=-1, keepdims=True)
        normed = centered * lax.rsqrt(variance + 1e-06) * gain + bias
        for f in range(vit // LANES):
            norm_buf[f] = normed[:, f * LANES:(f + 1) * LANES]

    def merge_rows(i, norm_buf):
        for j in range(per_token):
            strips = [norm_buf[f, pl.ds(j, ln_tokens, stride=per_token), :] for f in range(vit // LANES)]
            merged[j, pl.ds(pl.multiple_of(i * ln_tokens, ln_tokens), ln_tokens), :] = jnp.concatenate(strips, axis=1).astype(BF16)

    def norm_pair(h, carry):
        for i in (2 * h, 2 * h + 1):

            @pl.when(i < chunks)
            def _(i=i):
                first_copy(i).start()

        @pl.when(h == ln_steps // 2 - 1)
        def _():
            second_copy.start()
            text_copy.start()

        norm_rows(2 * h, norm_a)
        norm_rows(2 * h + 1, norm_b)
        merge_rows(2 * h, norm_a)
        merge_rows(2 * h + 1, norm_b)
        return carry

    lax.fori_loop(0, ln_steps // 2, norm_pair, 0)
    for table in tables:
        table.wait()

    token_row = lax.broadcasted_iota(jnp.int32, (rows, tokens), 0)
    token_gap = lax.broadcasted_iota(jnp.int32, (rows, tokens), 1) - token_row
    picked = jnp.zeros((rows, tokens), jnp.bool_)
    for b in range(strides):
        offset = routing_ref[b, me]
        start = jnp.int32(0)
        for o in range(strides):
            start = start + jnp.where(routing_ref[o, me] < offset, area_of(grids_ref, me, o), 0)
        stop = start + area_of(grids_ref, me, b)
        picked = picked | ((token_row >= start) & (token_row < stop) & (token_gap == b * cap - start))
    own_pick[...] = picked.astype(F32).astype(BF16)

    pl.semaphore_wait(barrier, greeted)

    def hidden_chunk(c):
        first_copy(c).wait()

        def add(j, carry):
            weight = first_buf[c, pl.ds(pl.multiple_of(j * vit, vit), vit), :]
            term = jnp.dot(merged[j], weight, preferred_element_type=F32)
            acc[...] = jnp.where(j == 0, term, acc[...] + term)
            return carry

        lax.fori_loop(0, per_token, add, 0)
        x = acc[...] + first_bias_ref[pl.ds(pl.multiple_of(c * CHUNK, CHUNK), CHUNK)][None, :]
        hidden = (0.5 * x * (1.0 + lax.erf(x * (0.5 ** 0.5)))).astype(BF16)
        gath[me, c] = jnp.dot(own_pick[...], hidden, preferred_element_type=F32).astype(BF16)

    def line_copy(block, c, way):
        here = gath.at[2 * block + row, c]
        return pltpu.make_async_remote_copy(
            src_ref=here,
            dst_ref=here,
            send_sem=line_send.at[(way + 1) // 2, block, c],
            recv_sem=line_recv.at[block, c],
            device_id={"dp": me + 2 * way},
        )

    def by_line(block, c):
        first = (block == 0) & (place != 0) & ((c >= cut) | (place == 1))
        last = (block == length - 1) & (place != length - 1) & ((c >= cut) | (place == length - 2))
        return first | last

    def extra_copy(c, way):
        here = gath.at[(length - 1) * (1 - way) + 1 - row, c]
        return pltpu.make_async_remote_copy(
            src_ref=here,
            dst_ref=here,
            send_sem=extra_send.at[(way + 1) // 2, c],
            recv_sem=extra_recv.at[(way + 1) // 2, c],
            device_id={"dp": me + 2 * way},
        )

    def pair_copy(block, c, side_row):
        here = gath.at[2 * block + side_row, c]
        return pltpu.make_async_remote_copy(
            src_ref=here,
            dst_ref=here,
            send_sem=pair_send.at[block, c],
            recv_sem=pair_recv.at[block, c],
            device_id={"dp": other},
        )

    def swap_copy(e, slot):
        return pltpu.make_async_remote_copy(
            src_ref=part.at[e, mate if slot == 0 else across_mate],
            dst_ref=pair_in.at[e, slot],
            send_sem=swap_send.at[slot, e],
            recv_sem=swap_recv.at[slot, e],
            device_id={"tensor": mate},
        )

    def cross_copy(e):
        return pltpu.make_async_remote_copy(
            src_ref=cross_out.at[e],
            dst_ref=cross_in.at[e],
            send_sem=cross_send.at[e],
            recv_sem=cross_recv.at[e],
            device_id={"tensor": across},
        )

    def place_of(source, sender):
        if by_columns:
            at = ((source % per_group) * groups + sender) * piece_cols
            return pl.ds(0, rows), pl.ds(pl.multiple_of(at, piece_cols), piece_cols)
        return (
            pl.ds(pl.multiple_of(sender * piece_rows, piece_rows), piece_rows),
            pl.ds(pl.multiple_of((source % per_group) * piece_cols, piece_cols), piece_cols),
        )

    def out_copy(e, source, sender):
        return pltpu.make_async_remote_copy(
            src_ref=ready_buf.at[e],
            dst_ref=out_ref.at[place_of(source, sender)],
            send_sem=out_send.at[e],
            recv_sem=out_recv.at[sender, source % per_group],
            device_id={"dp": e, "tensor": target},
        )

    def compute_ready(e):
        last = jnp.int32(0)
        for k in range(strides):
            source = (e + shards - k) % shards
            away = jnp.abs(source // 2 - place) + jnp.abs(source % 2 - row)
            last = jnp.maximum(last, away)
        return last

    packed = jnp.int32(0)
    if shards <= 8:
        for e in range(shards):
            packed = packed + compute_ready(jnp.int32(e)) * (1 << (3 * e))

    def ready_step(e):
        return (packed >> (3 * e)) & 7 if shards <= 8 else compute_ready(e)

    def over_shards(body):
        def run(i, carry):
            body((me + 1 + i) % shards)
            return carry

        lax.fori_loop(0, shards, run, 0)

    def accumulate(source, c, slot):
        weight = second_buf[pl.ds(pl.multiple_of(c * CHUNK, CHUNK), CHUNK), :]
        term = jnp.dot(gath[source, c], weight, preferred_element_type=F32)
        sums[slot] = jnp.where(c == 0, term, sums[slot] + term)

    def pick(e):
        at_row = lax.broadcasted_iota(jnp.int32, (rows, rows), 0)
        gap = lax.broadcasted_iota(jnp.int32, (rows, rows), 1) - at_row
        laid = jnp.int32(0)
        total = None
        for k in range(strides):
            source = (e + shards - k) % shards
            count, start = segment(grids_ref, routing_ref, source, k)
            chosen = (at_row >= laid) & (at_row < laid + count) & (gap == start - laid)
            term = jnp.dot(chosen.astype(F32).astype(BF16), proj[source], preferred_element_type=F32)
            total = term if total is None else total + term
            laid = laid + count
        total = total.astype(BF16)
        for g in range(groups):
            if by_columns:
                part[e, g] = total[:, g * piece_cols:(g + 1) * piece_cols]
            else:
                part[e, g] = total[g * piece_rows:(g + 1) * piece_rows]
        for slot in (1, 0):
            swap_copy(e, slot).start()

    def cross(e):
        swap_copy(e, 1).wait_recv()
        cross_out[e] = (part[e, across].astype(F32) + pair_in[e, 1].astype(F32)).astype(BF16)
        cross_copy(e).start()

    def finish(e):
        swap_copy(e, 0).wait_recv()
        cross_copy(e).wait_recv()
        total = (part[e, group].astype(F32) + pair_in[e, 0].astype(F32) + cross_in[e].astype(F32)).astype(BF16)

        stays = (e == me) & (target == group)

        @pl.when(jnp.logical_not(stays))
        def _():
            ready_buf[e] = total
            out_copy(e, me, group).start()

        @pl.when(stays)
        def _():
            at_rows, at_cols = place_of(me, group)
            out_ref[at_rows, at_cols] = total

    def row_sums(values):
        squares = values * values
        lanes = squares[:, :LANES]
        for f in range(1, feature // LANES):
            lanes = lanes + squares[:, f * LANES:(f + 1) * LANES]
        return jnp.sum(lanes.T, axis=0, keepdims=True)

    def text_sums():
        text_copy.wait()

        def block(i, carry):
            span = pl.ds(pl.multiple_of(i * LANES, LANES), LANES)
            sums_out[:, span] = row_sums(embed_ref[span, :].astype(F32))
            return carry

        lax.fori_loop(0, seq // LANES, block, 0)

    def is_block(block, away, way):
        return (away >= 0) & (away < length) & ((away > 0) | (way == 1)) & (block >= 0) & (block < length)

    def slot_step(step, c):
        @pl.when(step == 0)
        def _():
            hidden_chunk(c)

        for way in (1, -1):
            block = place - way * step
            have = (step < length) & (block >= 0) & (block < length)

            @pl.when(have & (step > 0))
            def _(block=block, way=way):
                line_copy(block, c, way).wait_recv()

            @pl.when(have & (place + way >= 0) & (place + way < length))
            def _(block=block, way=way):
                line_copy(block, c, way).start()

            @pl.when(is_block(block, step, way) & jnp.logical_not(by_line(block, c)))
            def _(block=block):
                pair_copy(block, c, row).start()

        def extras():
            for way in (1, -1):
                away = place if way == 1 else length - 1 - place

                chunk = c + jnp.where(away == 1, 0, cut)

                @pl.when((away > 0) & (step == away + 1) & (chunk < chunks))
                def _(away=away, way=way, chunk=chunk):
                    extra_copy(chunk, way).wait_recv()

                    @pl.when((away < length - 1) & (chunk >= cut))
                    def _():
                        extra_copy(chunk, way).start()

        @pl.when(step < length)
        def _():
            extras()

        @pl.when((step == 1) & (c == 0))
        def _():
            second_copy.wait()

        @pl.when((step == 1) & (c == 3))
        def _():
            text_sums()

        closing = (step == length) & (c >= cut)
        wanted = jnp.where(closing, length, step - 1)
        turn = jnp.where(closing, c - cut, c)

        @pl.when((step > 0) & (turn > 0) & (turn < 3))
        def _():
            def now(e):
                @pl.when((ready_step(e) == wanted) & ((e + row) % 2 == turn - 1))
                def _():
                    cross(e)

            over_shards(now)

        @pl.when((step > 0) & (turn < 2) & ((c < 2) | closing))
        def _():
            def now(e):
                @pl.when((ready_step(e) == wanted) & ((e + row) % 2 == turn))
                def _():
                    pick(e)

            over_shards(now)

        @pl.when(step == length)
        def _():
            extras()

        @pl.when((step == length) & (c == 3))
        def _():
            def now(e):
                @pl.when((ready_step(e) <= length - 2) & ((e + row) % 2 == 0))
                def _():
                    finish(e)

            over_shards(now)

        def unit(i, carry):
            way = 1 - 2 * (i % 2)
            own = i == 2
            block = jnp.where(own, place, place - way * step)

            @pl.when((step > 0) & jnp.where(own, step == 1, (step < length) & (block >= 0) & (block < length)))
            def _():
                accumulate(2 * block + row, c, jnp.where(own, 4, (way + 1) // 2))

            return carry

        lax.fori_loop(0, 3, unit, 0)

        def other_unit(i, carry):
            way = 1 - 2 * (i % 2)
            block = place - way * (step - 1)
            far = i // 2
            plain = is_block(block, step - 1, way)
            split = ((block == 0) & (place != 0)) | ((block == length - 1) & (place != length - 1))
            near = (far == 0) & plain & jnp.logical_not(by_line(block, c))
            chunk = c + far * jnp.where(step == 2, 0, cut)

            @pl.when(near)
            def _():
                pair_copy(block, c, 1 - row).wait_recv()

            @pl.when(near | ((far == 1) & plain & split & (chunk < chunks)))
            def _():
                accumulate(2 * block + 1 - row, chunk, 2 + (way + 1) // 2)

            return carry

        lax.fori_loop(0, 4, other_unit, 0)

        for way, end in ((1, 0), (-1, length - 1)):

            @pl.when((step == 1) & (place == end))
            def _(way=way):
                extra_copy(c, way).start()

        @pl.when(c == jnp.where(step == length, cut - 1, chunks - 1))
        def _():
            def settle_unit(i, carry):
                way, kind = 1 - 2 * (i % 2), i // 2
                block = place - way * (step - kind)

                @pl.when(is_block(block, step - kind, way) & (step > 0))
                def _():
                    source = 2 * block + jnp.abs(row - kind)
                    proj[source] = sums[2 * kind + (way + 1) // 2].astype(BF16)

                return carry

            lax.fori_loop(0, 4, settle_unit, 0)

            @pl.when(step == 1)
            def _():
                proj[me] = sums[4].astype(BF16)

    def outer(step, carry):
        def inner(c, carry):
            slot_step(step, c)
            return carry

        return lax.fori_loop(0, chunks, inner, carry)

    lax.fori_loop(0, length + 1, outer, 0)

    def last_cross(e):
        @pl.when((ready_step(e) == length) & ((e + row) % 2 == 1))
        def _():
            cross(e)

    over_shards(last_cross)

    def last_sends(i, carry):
        e, turn = (me + 1 + i) % shards, i // shards
        far, crosses = (e + row) % 2, ready_step(e)
        when = jnp.where(crosses == length, 3, jnp.where(crosses == length - 1, 0, 1 - 2 * (1 - far))) + jnp.where(crosses == length - 1, 2 * far, far * (crosses == length).astype(jnp.int32))

        @pl.when(when == turn)
        def _():
            finish(e)

        return carry

    lax.fori_loop(0, 5 * shards, last_sends, 0)

    filled = jnp.int32(0)
    for k in range(strides):
        filled = filled + segment(grids_ref, routing_ref, (me + shards - k) % shards, k)[0]
    lane_sums[...] = jnp.zeros_like(lane_sums)

    def splice(i, carry):
        sender, source = i % groups, group * per_group + i // groups

        @pl.when((sender != group) | (source != me))
        def _():
            out_copy(me, source, sender).wait_recv()

        at_rows, at_cols = place_of(source, sender)
        line = lax.broadcasted_iota(jnp.int32, (piece_rows, piece_cols), 0) + (0 if by_columns else sender * piece_rows)
        image = (out_ref[at_rows, at_cols].astype(F32) + second_bias_ref[at_cols][None, :]).astype(BF16)
        values = image.astype(F32)
        embed_ref[at_rows, at_cols] = jnp.where(line < filled, values, embed_ref[at_rows, at_cols].astype(F32)).astype(BF16)
        squares = values * values
        lanes = squares[:, :LANES]
        for f in range(1, piece_cols // LANES):
            lanes = lanes + squares[:, f * LANES:(f + 1) * LANES]
        lane_sums[at_rows, :] = lane_sums[at_rows, :] + lanes
        return carry

    lax.fori_loop(0, shards, splice, 0)
    for i in range(top_rows // LANES):
        span = slice(i * LANES, (i + 1) * LANES)
        line = lax.broadcasted_iota(jnp.int32, (1, LANES), 1) + i * LANES
        image = jnp.sum(lane_sums[span, :].T, axis=0, keepdims=True)
        sums_out[:, span] = jnp.where(line < filled, image, sums_out[:, span])

    def sums_copy(peer, sender, i):
        return pltpu.make_async_remote_copy(
            src_ref=sums_out,
            dst_ref=sums_in.at[sender],
            send_sem=sums_send.at[i],
            recv_sem=sums_recv.at[sender],
            device_id={"tensor": peer},
        )

    for i, peer in enumerate(peers):
        sums_copy(peer, group, i).start()

    def drain_line(t, carry):
        block, c = t // chunks, t % chunks

        @pl.when(jnp.logical_not(by_line(block, c)))
        def _():
            pair_copy(block, c, row).wait_send()

        @pl.when((block <= place) & (place < length - 1))
        def _():
            line_copy(block, c, 1).wait_send()

        @pl.when((block >= place) & (place > 0))
        def _():
            line_copy(block, c, -1).wait_send()

        return carry

    lax.fori_loop(0, length * chunks, drain_line, 0)

    def drain_extra(c, carry):
        for way, start, end in ((1, 0, length - 1), (-1, length - 1, 0)):

            @pl.when((place != end) & ((c >= cut) | (place == start)))
            def _(way=way):
                extra_copy(c, way).wait_send()

        return carry

    lax.fori_loop(0, chunks, drain_extra, 0)

    def drain(e):
        for slot in (1, 0):
            swap_copy(e, slot).wait_send()
        cross_copy(e).wait_send()

        @pl.when((e != me) | (target != group))
        def _():
            out_copy(e, me, group).wait_send()

    over_shards(drain)
    total = sums_out[...]
    for i, peer in enumerate(peers):
        copy = sums_copy(peer, peer, i)
        copy.wait_recv()
        copy.wait_send()
        total = total + sums_in[peer]
    sums_ref[...] = total


def merge(rows, call_id, shards, groups, grids, routing, patches, norm_gain, norm_bias, first_weight, first_bias, second_weight, second_bias, text_embeds):
    patch_rows, vit = patches.shape
    per_token = first_weight.shape[0] // vit
    tokens = patch_rows // per_token
    hidden_width = first_weight.shape[1]
    chunks = hidden_width // CHUNK
    depth, width = second_weight.shape
    seq, feature = text_embeds.shape
    length = shards // 2
    by_columns = width % (groups * LANES) == 0
    piece = (rows, width // groups) if by_columns else (rows // groups, width)
    per_group = shards // groups
    dma = pltpu.SemaphoreType.DMA
    vmem = pl.BlockSpec(memory_space=pltpu.VMEM)
    anywhere = pl.BlockSpec(memory_space=pl.ANY)
    block = pltpu.VMEM((shards,) + piece, BF16)
    return pl.pallas_call(
        functools.partial(merge_kernel, rows, by_columns),
        in_specs=[anywhere, anywhere, anywhere, vmem, vmem, anywhere, vmem, anywhere, vmem, anywhere],
        out_specs=[vmem, vmem],
        out_shape=[
            jax.ShapeDtypeStruct((seq, feature), BF16),
            jax.ShapeDtypeStruct((1, seq), F32),
        ],
        scratch_shapes=[
            pltpu.SMEM(grids.shape, jnp.int32),
            pltpu.SMEM(routing.shape, jnp.int32),
            pltpu.VMEM((tokens, LANES), F32),
            pltpu.VMEM((tokens, feature), BF16),
            pltpu.VMEM((patch_rows, vit), BF16),
            pltpu.VMEM((vit // LANES, LANES, LANES), F32),
            pltpu.VMEM((vit // LANES, LANES, LANES), F32),
            pltpu.VMEM((per_token, tokens, vit), BF16),
            pltpu.VMEM((chunks, first_weight.shape[0], CHUNK), BF16),
            pltpu.VMEM((depth, width), BF16),
            pltpu.VMEM((rows, tokens), BF16),
            pltpu.VMEM((tokens, CHUNK), F32),
            pltpu.VMEM((shards, chunks, rows, CHUNK), BF16),
            pltpu.VMEM((5, rows, width), F32),
            pltpu.VMEM((shards, rows, width), BF16),
            pltpu.VMEM((shards, groups) + piece, BF16),
            pltpu.VMEM((shards, 2) + piece, BF16),
            block, block, block,
            pltpu.VMEM((1, seq), F32),
            pltpu.VMEM((groups, 1, seq), F32),
            dma((2,)), dma((patch_rows // LANES,)), dma((chunks,)), dma, dma,
            dma((2, length, chunks)), dma((length, chunks)), dma((2, chunks)), dma((2, chunks)),
            dma((length, chunks)), dma((length, chunks)),
            dma((2, shards)), dma((2, shards)), dma((shards,)), dma((shards,)),
            dma((shards,)), dma((groups, per_group)),
            dma((groups - 1,)), dma((groups,)),
        ],
        compiler_params=pltpu.CompilerParams(
            collective_id=call_id, has_side_effects=True, vmem_limit_bytes=VMEM_LIMIT
        ),
        name="merge_%d" % rows,
    )(grids, routing, patches, norm_gain, norm_bias, first_weight, first_bias, second_weight, second_bias, text_embeds)


def scale_kernel(total_width, embed_ref, sums_ref, gain_ref, out_ref, normed_ref, normed_buf, out_sem, normed_sem):
    feature = gain_ref.shape[0]
    blocks = normed_buf.shape[0]
    out_copy = pltpu.make_async_copy(embed_ref, out_ref, out_sem)
    out_copy.start()

    def normed_copy(i):
        return pltpu.make_async_copy(normed_buf.at[i], normed_ref.at[pl.ds(i * LANES, LANES)], normed_sem.at[i])

    for i in range(blocks):
        span = slice(i * LANES, (i + 1) * LANES)
        scale = lax.rsqrt(sums_ref[:, span] / total_width + 1e-06)
        scale = jnp.broadcast_to(scale, (LANES, LANES)).T
        for f in range(feature // LANES):
            at = slice(f * LANES, (f + 1) * LANES)
            normed_buf[i, :, at] = (embed_ref[span, at].astype(F32) * scale * gain_ref[at][None, :]).astype(BF16)
        normed_copy(i).start()

    out_copy.wait()
    for i in range(blocks):
        normed_copy(i).wait()


def scale_rows(embeddings, sums, final_gain, groups):
    seq, feature = embeddings.shape
    anywhere = pl.BlockSpec(memory_space=pl.ANY)
    vmem = pl.BlockSpec(memory_space=pltpu.VMEM)
    blocks = seq // LANES
    dma = pltpu.SemaphoreType.DMA
    return pl.pallas_call(
        functools.partial(scale_kernel, feature * groups),
        in_specs=[vmem, vmem, vmem],
        out_specs=[anywhere, anywhere],
        out_shape=[jax.ShapeDtypeStruct((seq, feature), BF16)] * 2,
        scratch_shapes=[pltpu.VMEM((blocks, LANES, feature), BF16), dma, dma((blocks,))],
        compiler_params=pltpu.CompilerParams(vmem_limit_bytes=VMEM_LIMIT),
        name="scale_rows",
    )(embeddings, sums, final_gain)


def bucket_sizes(slots, width, groups):
    step = slots // 16 if width % (groups * LANES) == 0 else slots // 4
    return tuple(b for b in range(slots // 2 + step, slots + 1, step) if b <= slots * 13 // 16 or b == slots)


def per_device(
    patches,
    norm_gain,
    norm_bias,
    first_weight,
    first_bias,
    second_weight,
    second_bias,
    text_embeds,
    final_gain,
    image_grids,
    routing,
):
    shards = lax.axis_size("dp")
    groups = lax.axis_size("tensor")
    slots = patches.shape[0] * patches.shape[1] // first_weight.shape[0]
    grids, offsets = image_grids.transpose(1, 2, 0), routing.T
    buckets = BUCKETS(slots, second_weight.shape[1], groups)
    which = pl.pallas_call(
        functools.partial(plan_kernel, buckets),
        in_specs=[pl.BlockSpec(memory_space=pl.ANY)] * 2,
        out_specs=pl.BlockSpec(memory_space=pltpu.SMEM),
        out_shape=jax.ShapeDtypeStruct((1,), jnp.int32),
        scratch_shapes=[
            pltpu.SMEM(grids.shape, jnp.int32),
            pltpu.SMEM(offsets.shape, jnp.int32),
            pltpu.SMEM((shards,), jnp.int32),
            pltpu.SemaphoreType.DMA((2,)),
        ],
        name="plan",
    )(grids, offsets)

    def branch(rows, call_id):
        return lambda: merge(
            rows, call_id, shards, groups, grids, offsets, patches, norm_gain, norm_bias,
            first_weight, first_bias, second_weight, second_bias, text_embeds,
        )

    embeddings, sums = lax.switch(which[0], [branch(rows, i) for i, rows in enumerate(buckets)])
    return tuple(scale_rows(embeddings, sums, final_gain, groups))


BUCKETS = bucket_sizes


def solution(mesh):
    placed = (
        P("dp", None),
        P(),
        P(),
        P(None, "tensor"),
        P("tensor"),
        P("tensor", "dp"),
        P("tensor"),
        P("dp", "tensor"),
        P("tensor"),
        P(),
        P(),
    )
    return jax.shard_map(
        per_device,
        mesh=mesh,
        in_specs=placed,
        out_specs=(P("dp", "tensor"), P("dp", "tensor")),
        check_vma=False,
    )
```
